256 devices in a mesh: row: 2 (over core), col: 4 (over x), depth: 32 (over z, y).
Axes of the slice: x: 4, y: 4, z: 8, core: 2. Of those that a mesh axis runs over, the one named last changes fastest.
Arguments:
- a_tile: float32 [2048, 2048], P('row', 'col'), as said below
- panels: float32 [2048, 32768], P('row', 'depth'), as said below
Outputs:
- trailing: float32 [2048, 2048], P(('row', 'depth'), 'col')
- new_panel: float32 [2048, 512], P(('row', 'col'))
- diag_norm: float32 [1], replicated
Inputs may be any that keep to these rules, and one draw needn't show every extreme that they name: symmetric; a_tile - panels panels^T is positive definite with a large positive diagonal. `panels`: real-valued entries of full rank.
All inputs are finite; a program needn't handle non-finite values.
Results may differ from the reference program's by a relative error of at most 0.00015.
Values sent between devices are 32-bit elements; how exact they have to be, the bound alone decides.
No kernel may reach another device: no remote copies, remote signals or barrier semaphores. Data moves between devices by JAX's collectives and lax.ppermute only.
A program may use at most 64 MiB of HBM per device.

```python
import jax
import jax.numpy as jnp
from jax import lax

PB = 512
M = 2048
KTOT = 32768


def panel_matrix(key):
    key_panel = jax.random.fold_in(key, 21)
    deviation = jnp.sqrt(1.5 / jnp.sqrt(jnp.float32(M) * jnp.float32(KTOT)))
    base = jnp.clip(jax.random.normal(key_panel, (M, KTOT), jnp.float32), -6.0, 6.0)
    return (base * deviation).astype(jnp.float32)


def draw_panels(key, part):
    return panel_matrix(key)


def draw_a_tile(key, part):
    key_noise = jax.random.fold_in(key, 11)
    key_diag = jax.random.fold_in(key, 12)
    noise = jax.random.normal(key_noise, (M, M), jnp.float32)
    spread = jax.random.uniform(key_diag, (M,), jnp.float32, 1.0, 1.5)
    noise = noise * (0.5 / jnp.sqrt(jnp.float32(M)))
    symmetric = (noise + noise.T) * 0.7071
    rising = jnp.power(3.0, jnp.arange(M, dtype=jnp.float32) / M)
    diagonal = 4.0 * rising * spread
    panel_full = panel_matrix(key)
    product = jnp.dot(panel_full, panel_full.T, precision=lax.Precision.HIGHEST, preferred_element_type=jnp.float32)
    product = (product + product.T) * 0.5
    return (symmetric + jnp.diag(diagonal) + product).astype(jnp.float32)


def setup_inputs(seed: int = 0) -> dict:
    splits = jax.random.split(jax.random.key(seed), 3)
    a_tile = draw_a_tile(jax.random.fold_in(splits[2], 71), 0)
    panels = draw_panels(jax.random.fold_in(splits[2], 71), 0)
    return dict(a_tile=a_tile, panels=panels)


def reference(a_tile, panels):
    product = jnp.dot(panels.astype(jnp.float32), panels.T.astype(jnp.float32), precision=lax.Precision.HIGHEST, preferred_element_type=jnp.float32)
    trailing = a_tile - product
    factor = jnp.linalg.cholesky(trailing[:PB, :PB])
    new_panel = jax.scipy.linalg.solve_triangular(factor, trailing[:, :PB].T, lower=True).T
    diagonal = jnp.diagonal(trailing)
    diag_norm = jnp.sqrt(jnp.sum(diagonal * diagonal) / M).reshape(1)
    return (trailing, new_panel, diag_norm)
```

```python
import jax
import jax.numpy as jnp
from jax import lax
from jax.experimental import pallas as pl
from jax.experimental.pallas import tpu as pltpu
from jax.sharding import Mesh
from jax.sharding import PartitionSpec as P

PB = 512
LANES = 128
SUBLANES = 8
GROUPS = LANES // SUBLANES
BLOCKS = PB // LANES
PAIRS = BLOCKS * (BLOCKS + 1) // 2
DEPTH = ("depth_0", "depth_1")
ROW_DEPTH = ("row", "depth_0", "depth_1")
F32 = jnp.float32


def times_transposed(left, right):
    return lax.dot_general(
        left,
        right,
        (((1,), (1,)), ((), ())),
        precision=lax.Precision.HIGHEST,
        preferred_element_type=F32,
    )


def pair(i, j):
    return i * (i + 1) // 2 + j


def inverse_factor(load, store):
    lane = lax.broadcasted_iota(jnp.int32, (SUBLANES, LANES), 1)
    sub = lax.broadcasted_iota(jnp.int32, (SUBLANES, LANES), 0)
    whole = (SUBLANES, LANES)
    rows = [load(h) for h in range(GROUPS)]
    for g in range(GROUPS):
        first = SUBLANES * g
        cols = {
            h: [
                jnp.broadcast_to(rows[h][:, first + j : first + j + 1], whole)
                for j in range(SUBLANES)
            ]
            for h in range(g, GROUPS)
        }
        inside = (lane >= first) & (lane < first + SUBLANES)
        rows[g] = jnp.where(inside, jnp.where(lane - first == sub, 1.0, 0.0), rows[g])
        for h in range(g + 1, GROUPS):
            rows[h] = jnp.where(inside, 0.0, rows[h])
        done = jnp.zeros(whole, F32)
        for j in range(SUBLANES):
            scale = lax.rsqrt(jnp.broadcast_to(cols[g][j][j : j + 1], whole))
            row = jnp.broadcast_to(rows[g][j : j + 1], whole) * scale
            done = jnp.where(sub == j, row, done)
            own = cols[g][j] * scale
            spread = {
                k: jnp.broadcast_to(own[k : k + 1], whole) for k in range(j + 1, SUBLANES)
            }
            for k in spread:
                cols[g][k] = cols[g][k] - own * spread[k]
            rows[g] = rows[g] - jnp.where(sub > j, own, 0.0) * row
            for h in range(g + 1, GROUPS):
                below = cols[h][j] * scale
                rows[h] = rows[h] - below * row
                for k in spread:
                    cols[h][k] = cols[h][k] - below * spread[k]
        store(g, jnp.where(lane <= first + sub, done, 0.0))


def solve_kernel(top_ref, mine_ref, other_ref, c_ref, x_ref, w, inv_ref):
    pieces, per_piece = mine_ref.shape[0], PAIRS * GROUPS // mine_ref.shape[0]
    top = top_ref[0] == 0
    for ref, mine in ((mine_ref, top), (other_ref, jnp.logical_not(top))):

        @pl.when(mine)
        def _(ref=ref):
            for t in range(pieces * per_piece):
                b, h = t // GROUPS, t % GROUPS
                w[b, SUBLANES * h : SUBLANES * (h + 1)] = ref[t // per_piece, t % per_piece]

    x_ref[...] = c_ref[...]

    def step(b, carry):
        diag = (b * (b + 3)) // 2

        def load(h):
            return w[diag, SUBLANES * h : SUBLANES * (h + 1)]

        def store(h, value):
            inv_ref[SUBLANES * h : SUBLANES * (h + 1)] = value

        inverse_factor(load, store)
        for s in range(BLOCKS):

            @pl.when(b == s)
            def _(s=s):
                inv = inv_ref[...]
                here = slice(LANES * s, LANES * (s + 1))
                for i in range(s + 1, BLOCKS):
                    w[pair(i, s)] = times_transposed(w[pair(i, s)], inv)
                x = times_transposed(x_ref[:, here], inv)
                x_ref[:, here] = x
                for j in range(s + 1, BLOCKS):
                    there = slice(LANES * j, LANES * (j + 1))
                    for i in range(j, BLOCKS):
                        w[pair(i, j)] = w[pair(i, j)] - times_transposed(w[pair(i, s)], w[pair(j, s)])
                    x_ref[:, there] = x_ref[:, there] - times_transposed(x, w[pair(j, s)])

        return carry

    lax.fori_loop(0, BLOCKS, step, 0)


def solve(row_index, mine, other, c_rows):
    vmem = pl.BlockSpec(memory_space=pltpu.VMEM)
    return pl.pallas_call(
        solve_kernel,
        out_shape=jax.ShapeDtypeStruct(c_rows.shape, F32),
        in_specs=[pl.BlockSpec(memory_space=pltpu.SMEM), vmem, vmem, vmem],
        out_specs=vmem,
        scratch_shapes=[
            pltpu.VMEM((PAIRS, LANES, LANES), F32),
            pltpu.VMEM((LANES, LANES), F32),
        ],
        cost_estimate=pl.CostEstimate(flops=20_000_000_000, bytes_accessed=3_000_000, transcendentals=512),
        name="panel_solve",
    )(row_index.reshape(1).astype(jnp.int32), mine, other, c_rows)


def exchange(pieces, axis):
    return lax.all_to_all(pieces, axis, split_axis=0, concat_axis=0, tiled=True)


def to_everyone(value, axis):
    size = lax.axis_size(axis)
    return exchange(jnp.broadcast_to(value[None], (size, *value.shape)), axis)


def packed(square):
    return jnp.concatenate(
        [
            square[LANES * i : LANES * (i + 1), LANES * j : LANES * (j + 1)]
            for i in range(BLOCKS)
            for j in range(i + 1)
        ]
    )


def first_row_of_tile(values):
    n, k = values.shape
    return jnp.pad(values[:, None, None, :], ((0, 0), (0, 0), (0, SUBLANES - 1), (0, LANES - k)))


def local(a_tile, panels):
    tile_rows, tile_cols = a_tile.shape
    rows, cols = lax.axis_size("row"), lax.axis_size("col")
    depth = lax.axis_size(DEPTH)
    z_size, y_size = lax.axis_size("depth_0"), lax.axis_size("depth_1")
    r, c, d = lax.axis_index("row"), lax.axis_index("col"), lax.axis_index(DEPTH)
    share = tile_rows // depth
    c_rows = tile_rows // cols
    c_share = c_rows // depth
    tiles = PAIRS * GROUPS // depth

    a_share = lax.dynamic_slice_in_dim(a_tile, d * share, share, 0)
    a_diag = lax.dynamic_slice_in_dim(packed(a_tile[:PB]), d * tiles * SUBLANES, tiles * SUBLANES, 0)
    a_panel = lax.dynamic_slice_in_dim(a_tile.reshape(cols, c_rows, tile_cols), d * c_share, c_share, 1)
    row0 = r * tile_rows + d * share
    holder = row0 // tile_cols == c
    square = lax.dynamic_slice_in_dim(a_share, row0 % tile_cols, share, 1)
    a_ii = jnp.sum(jnp.where(jnp.eye(share, dtype=bool), square, 0.0), axis=0)
    a_ii = first_row_of_tile(jnp.where(holder, a_ii, 0.0)[None])[0]
    same = jnp.concatenate([a_diag.reshape(tiles, SUBLANES, LANES), a_ii])
    a_sent = jnp.concatenate(
        [
            jnp.broadcast_to(same[None], (cols, *same.shape)),
            a_panel.reshape(cols, c_share, tile_cols // LANES, LANES).transpose(0, 2, 1, 3),
        ],
        axis=1,
    )
    a_got = exchange(a_sent, "col")
    a_diag = a_got[0, :tiles]
    a_ii = a_got[:, tiles].sum(axis=0)
    a_panel = a_got[0, tiles + 1 :].transpose(1, 0, 2).reshape(c_share, tile_cols)

    swap = [(0, 1), (1, 0)]
    far = lax.ppermute(panels[:PB], "row", swap)
    far_rest = lax.ppermute(panels[PB:], "row", swap)

    near = panels[:PB]
    part = packed(times_transposed(near, near)).reshape(depth, tiles, SUBLANES, LANES)
    part_ii = jnp.sum(panels * panels, axis=1).reshape(depth, share)
    got = exchange(jnp.concatenate([part, first_row_of_tile(part_ii)], axis=1), DEPTH).sum(axis=0)
    diag_ii = a_ii - got[tiles]
    total = jnp.sum(diag_ii * diag_ii)
    piece = jnp.concatenate([a_diag - got[:tiles], jnp.broadcast_to(total, (1, SUBLANES, LANES))])
    mine = to_everyone(piece, DEPTH)
    other = lax.ppermute(mine, "row", swap)
    total = jnp.sum(mine[:, tiles, 0, 0]) + jnp.sum(other[:, tiles, 0, 0])
    diag_norm = jnp.sqrt(total / (rows * tile_rows)).reshape(1)

    top = jnp.where(r == 0, near, far)
    own = lax.dynamic_slice_in_dim(panels, c * c_rows, c_rows, 0)
    c_part = times_transposed(own, top).reshape(depth, c_share, tile_cols)
    c_piece = a_panel - exchange(c_part, DEPTH).sum(axis=0)
    c_all = to_everyone(c_piece, DEPTH).reshape(c_rows, tile_cols)

    first = c * tile_cols
    here = first // tile_rows == r
    half = first % tile_rows // PB
    right = jnp.where(
        here,
        lax.dynamic_slice_in_dim(panels, half * PB, PB, 0),
        jnp.where(half == 0, far, far_rest),
    )
    block = times_transposed(panels, right)
    block = block.reshape(z_size, y_size, share, tile_cols).transpose(1, 0, 2, 3)
    block = exchange(block, "depth_1").sum(axis=0)
    trailing = a_share - exchange(block, "depth_0").sum(axis=0)

    new_panel = solve(r, mine, other, c_all)
    return (trailing, new_panel, diag_norm)


def solution(mesh):
    finer = Mesh(
        mesh.devices.reshape(mesh.shape["row"], mesh.shape["col"], 8, 4),
        ("row", "col", "depth_0", "depth_1"),
    )
    in_specs = (P("row", "col"), P("row", DEPTH))
    out_specs = (P(ROW_DEPTH, "col"), P(("row", "col"), None), P())
    return jax.shard_map(local, mesh=finer, in_specs=in_specs, out_specs=out_specs, check_vma=False)
```

```python
import jax
import jax.numpy as jnp
from jax import lax
from jax.experimental import pallas as pl
from jax.experimental.pallas import tpu as pltpu
from jax.sharding import Mesh
from jax.sharding import PartitionSpec as P

PB = 512
LANES = 128
SUBLANES = 8
GROUPS = LANES // SUBLANES
TILE = (SUBLANES, LANES)
BLOCKS = PB // LANES
PAIRS = BLOCKS * (BLOCKS + 1) // 2
DEPTH = ("depth_0", "depth_1")
ROW_DEPTH = ("row", "depth_0", "depth_1")
Z, Y = DEPTH
Y_SIZE = 4
WIDE = PB // LANES
F32 = jnp.float32


def times_transposed(left, right):
    return lax.dot_general(
        left,
        right,
        (((1,), (1,)), ((), ())),
        precision=lax.Precision.HIGHEST,
        preferred_element_type=F32,
    )


def pair(i, j):
    return i * (i + 1) // 2 + j


def inverse_factor(load, store):
    lane = lax.broadcasted_iota(jnp.int32, (SUBLANES, LANES), 1)
    sub = lax.broadcasted_iota(jnp.int32, (SUBLANES, LANES), 0)
    whole = (SUBLANES, LANES)
    rows = [load(h) for h in range(GROUPS)]
    for g in range(GROUPS):
        first = SUBLANES * g
        cols = {
            h: [
                jnp.broadcast_to(rows[h][:, first + j : first + j + 1], whole)
                for j in range(SUBLANES)
            ]
            for h in range(g, GROUPS)
        }
        inside = (lane >= first) & (lane < first + SUBLANES)
        rows[g] = jnp.where(inside, jnp.where(lane - first == sub, 1.0, 0.0), rows[g])
        for h in range(g + 1, GROUPS):
            rows[h] = jnp.where(inside, 0.0, rows[h])
        done = jnp.zeros(whole, F32)
        for j in range(SUBLANES):
            scale = lax.rsqrt(jnp.broadcast_to(cols[g][j][j : j + 1], whole))
            row = jnp.broadcast_to(rows[g][j : j + 1], whole) * scale
            done = jnp.where(sub == j, row, done)
            own = cols[g][j] * scale
            spread = {
                k: jnp.broadcast_to(own[k : k + 1], whole) for k in range(j + 1, SUBLANES)
            }
            for k in spread:
                cols[g][k] = cols[g][k] - own * spread[k]
            rows[g] = rows[g] - jnp.where(sub > j, own, 0.0) * row
            for h in range(g + 1, GROUPS):
                below = cols[h][j] * scale
                rows[h] = rows[h] - below * row
                for k in spread:
                    cols[h][k] = cols[h][k] - below * spread[k]
        store(g, jnp.where(lane <= first + sub, done, 0.0))


def halves(value):
    high = value.astype(jnp.bfloat16)
    return high, (value - high.astype(F32)).astype(jnp.bfloat16)


def product(left, right):
    def dot(a, b):
        return lax.dot_general(a, b, (((1,), (1,)), ((), ())), preferred_element_type=F32)

    return dot(left[0], right[0]) + (dot(left[0], right[1]) + dot(left[1], right[0]))


def diag_kernel(place_ref, p_ref, *refs):
    outs, all_ref = refs[:Y_SIZE], refs[Y_SIZE]
    step = pl.program_id(0)
    y = place_ref[3]
    lane = lax.broadcasted_iota(jnp.int32, TILE, 1)
    sub = lax.broadcasted_iota(jnp.int32, TILE, 0)
    per_piece = PAIRS * GROUPS // 32
    p = p_ref[...]
    squares = halves(p * p)
    ones = jnp.ones((SUBLANES, p.shape[1]), jnp.bfloat16)

    def row_sums(part):
        return lax.dot_general(ones, part, (((1,), (1,)), ((), ())), preferred_element_type=F32)

    sums = row_sums(squares[0]) + row_sums(squares[1])
    for zz in range(WIDE):
        for yy in range(Y_SIZE):
            keep = (sub == 0) & (lane // 32 == yy)
            all_ref[yy, step * WIDE + zz, per_piece] = jnp.where(
                keep, sums[:, LANES * zz : LANES * (zz + 1)], 0.0
            )

    @pl.when(step == 0)
    def _():
        parts = halves(p)
        rows = [tuple(x[LANES * i : LANES * (i + 1)] for x in parts) for i in range(BLOCKS)]
        for i in range(BLOCKS):
            for j in range(i + 1):
                value = product(rows[i], rows[j])
                for h in range(GROUPS):
                    t = pair(i, j) * GROUPS + h
                    d, k = t // per_piece, t % per_piece
                    all_ref[d % Y_SIZE, d // Y_SIZE, k] = value[SUBLANES * h : SUBLANES * (h + 1)]

    @pl.when(step == 1)
    def _():
        for s in range(Y_SIZE):
            outs[s][...] = all_ref[lax.rem(y + s, Y_SIZE)]


def a_kernel(place_ref, a_ref, *refs):
    cols = 4
    outs = refs[:cols]
    tile_buf, panel_buf, own_buf, sem = refs[cols:]
    r, c, z, y = place_ref[0], place_ref[1], place_ref[2], place_ref[3]
    d = z * Y_SIZE + y
    per_piece = tile_buf.shape[0]
    copies = []
    for k in range(per_piece):
        t = d * per_piece + k
        b, h = t // GROUPS, lax.rem(t, GROUPS)
        i = (b >= 1).astype(jnp.int32) + (b >= 3).astype(jnp.int32) + (b >= 6).astype(jnp.int32)
        j = b - (i * (i + 1)) // 2
        row = pl.multiple_of(i * LANES + h * SUBLANES, SUBLANES)
        col = pl.multiple_of(j * LANES, LANES)
        copies.append((a_ref.at[pl.ds(row, SUBLANES), pl.ds(col, LANES)], tile_buf.at[k]))
    for s in range(cols):
        row = pl.multiple_of(lax.rem(c + s, cols) * 256 + d * SUBLANES, SUBLANES)
        copies.append((a_ref.at[pl.ds(row, SUBLANES), :], panel_buf.at[s]))
    row = pl.multiple_of(d * 32, 32)
    col = pl.multiple_of(lax.rem(z, WIDE) * LANES, LANES)
    copies.append((a_ref.at[pl.ds(row, 32), pl.ds(col, LANES)], own_buf))
    copies = [pltpu.make_async_copy(a, b, sem.at[n]) for n, (a, b) in enumerate(copies)]
    for copy in copies:
        copy.start()
    for copy in copies:
        copy.wait()
    lane = lax.broadcasted_iota(jnp.int32, (32, LANES), 1)
    sub = lax.broadcasted_iota(jnp.int32, (32, LANES), 0)
    diagonal = jnp.sum(jnp.where(lane == y * 32 + sub, own_buf[...], 0.0), axis=0, keepdims=True)
    holder = c == r * 2 + z // WIDE
    first = lax.broadcasted_iota(jnp.int32, TILE, 0) == 0
    diagonal = jnp.where(first & holder, jnp.broadcast_to(diagonal, TILE), 0.0)
    root = c == 0
    for s in range(cols):
        for k in range(per_piece):
            outs[s][k] = jnp.where(root, tile_buf[k], 0.0)
        outs[s][per_piece] = diagonal
        for l in range(WIDE):
            outs[s][per_piece + 1 + l] = jnp.where(
                root, panel_buf[s, :, LANES * l : LANES * (l + 1)], 0.0
            )


def panel_kernel(place_ref, own_ref, near_ref, far_ref, *refs):
    outs, top_ref, all_ref, sem = refs[:Y_SIZE], *refs[Y_SIZE:]
    r, y = place_ref[0], place_ref[3]

    @pl.when(r == 0)
    def _():
        pltpu.make_async_copy(near_ref.at[pl.ds(0, PB)], top_ref, sem).start()

    @pl.when(r != 0)
    def _():
        pltpu.make_async_copy(far_ref.at[pl.ds(0, PB)], top_ref, sem).start()

    left = halves(own_ref[...])
    pltpu.make_async_copy(near_ref.at[pl.ds(0, PB)], top_ref, sem).wait()
    for l in range(WIDE):
        value = product(left, halves(top_ref[LANES * l : LANES * (l + 1)]))
        for g in range(value.shape[0] // SUBLANES):
            all_ref[g % Y_SIZE, g // Y_SIZE, l] = value[SUBLANES * g : SUBLANES * (g + 1)]
    for s in range(Y_SIZE):
        outs[s][...] = all_ref[lax.rem(y + s, Y_SIZE)]


def block_kernel(place_ref, left_ref, near_ref, far_ref, *refs):
    outs, high_ref, low_ref, right_ref, sem = refs[:Y_SIZE], *refs[Y_SIZE:]
    r, c, y = place_ref[0], place_ref[1], place_ref[3]
    step = pl.program_id(0)
    here = c // 2 == r
    half = pl.multiple_of(lax.rem(c, 2) * PB, PB)

    @pl.when(step == 0)
    def _():
        @pl.when(here)
        def _():
            pltpu.make_async_copy(near_ref.at[pl.ds(half, PB)], right_ref, sem).start()

        @pl.when(jnp.logical_not(here))
        def _():
            pltpu.make_async_copy(far_ref.at[pl.ds(half, PB)], right_ref, sem).start()

        pltpu.make_async_copy(near_ref.at[pl.ds(half, PB)], right_ref, sem).wait()
        high, low = halves(right_ref[...])
        high_ref[...] = high
        low_ref[...] = low

    value = product(halves(left_ref[...]), (high_ref[...], low_ref[...]))
    for yy in range(Y_SIZE):
        for s in range(Y_SIZE):

            @pl.when(lax.rem(yy - y + Y_SIZE, Y_SIZE) == s)
            def _(yy=yy, s=s):
                for g in range(4):
                    for l in range(WIDE):
                        row = 32 * yy + SUBLANES * g
                        outs[s][0, g * WIDE + l] = value[
                            row : row + SUBLANES, LANES * l : LANES * (l + 1)
                        ]


def factor_kernel(place_ref, *refs):
    gathered, inverse_ref, norm_ref, w, inv_ref = refs[:Y_SIZE], *refs[Y_SIZE:]
    y = place_ref[3]
    z_size, per_piece = gathered[0].shape[0], gathered[0].shape[1] - 1
    total = jnp.zeros(TILE, F32)
    for s in range(Y_SIZE):
        source = lax.rem(y - s + Y_SIZE, Y_SIZE)
        for zz in range(z_size):
            for k in range(per_piece):
                t = (zz * Y_SIZE + source) * per_piece + k
                w[pl.ds(pl.multiple_of(t * SUBLANES, SUBLANES), SUBLANES)] = gathered[s][zz, k]
            total = total + gathered[s][zz, per_piece]
    norm_ref[...] = jnp.sqrt(total / 2048.0)

    def at(i, j):
        return slice(LANES * pair(i, j), LANES * (pair(i, j) + 1))

    def block(i):
        return slice(LANES * i, LANES * (i + 1))

    lane = lax.broadcasted_iota(jnp.int32, (PB, PB), 1)
    sub = lax.broadcasted_iota(jnp.int32, (PB, PB), 0)
    inverse_ref[...] = jnp.where(lane == sub, 1.0, 0.0)

    def step(b, carry):
        start = (b * (b + 3)) // 2 * LANES

        def load(h):
            return w[pl.ds(pl.multiple_of(start + SUBLANES * h, SUBLANES), SUBLANES)]

        def store(h, value):
            inv_ref[SUBLANES * h : SUBLANES * (h + 1)] = value

        inverse_factor(load, store)
        for s in range(BLOCKS):

            @pl.when(b == s)
            def _(s=s):
                inv = inv_ref[...]
                for i in range(s + 1, BLOCKS):
                    w[at(i, s)] = times_transposed(w[at(i, s)], inv)
                for j in range(s + 1, BLOCKS):
                    for i in range(j, BLOCKS):
                        w[at(i, j)] = w[at(i, j)] - times_transposed(w[at(i, s)], w[at(j, s)])
                top = slice(0, LANES * (s + 1))
                x = times_transposed(inverse_ref[top, block(s)], inv)
                inverse_ref[top, block(s)] = x
                for j in range(s + 1, BLOCKS):
                    inverse_ref[top, block(j)] = inverse_ref[top, block(j)] - times_transposed(
                        x, w[at(j, s)]
                    )

        return carry

    lax.fori_loop(0, BLOCKS, step, 0)


def solve_kernel(place_ref, inverse_ref, *refs):
    gathered, x_ref, c_ref = refs[:Y_SIZE], *refs[Y_SIZE:]
    y = place_ref[3]
    for s in range(Y_SIZE):
        source = lax.rem(y - s + Y_SIZE, Y_SIZE)
        for zz in range(gathered[s].shape[0]):
            row = pl.multiple_of((zz * Y_SIZE + source) * SUBLANES, SUBLANES)
            for l in range(WIDE):
                c_ref[pl.ds(row, SUBLANES), LANES * l : LANES * (l + 1)] = gathered[s][zz, l]
    for l in range(WIDE):
        deep = slice(0, LANES * (l + 1))
        here = slice(LANES * l, LANES * (l + 1))
        x_ref[:, here] = jnp.dot(
            c_ref[:, deep],
            inverse_ref[deep, here],
            precision=lax.Precision.HIGHEST,
            preferred_element_type=F32,
        )


SMEM = pl.BlockSpec(memory_space=pltpu.SMEM)
VMEM = pl.BlockSpec(memory_space=pltpu.VMEM)
ANY = pl.BlockSpec(memory_space=pl.ANY)


def shaped(*dims):
    return jax.ShapeDtypeStruct(dims, F32)


def call(kernel, name, flops, outs, in_specs, scratch=(), grid=(), out_spec=None):
    out_specs = [out_spec or VMEM] * len(outs)
    return pl.pallas_call(
        kernel,
        name=name,
        out_shape=outs,
        grid=grid,
        in_specs=in_specs,
        out_specs=out_specs,
        scratch_shapes=scratch,
        cost_estimate=pl.CostEstimate(flops=flops, bytes_accessed=4_000_000, transcendentals=0),
    )


def exchange(pieces, axis):
    return lax.all_to_all(pieces, axis, split_axis=0, concat_axis=0, tiled=True)


def shifted(value, axis, by):
    size = lax.axis_size(axis)
    return lax.ppermute(value, axis, [(i, (i + by) % size) for i in range(size)])


def delivered(pieces, axis):
    return [pieces[0]] + [shifted(pieces[s], axis, s) for s in range(1, len(pieces))]


def gathered(value, axis):
    return delivered([value] * lax.axis_size(axis), axis)


def local(a_tile, panels):
    tile_rows, tile_cols = a_tile.shape
    z_size = lax.axis_size(Z)
    c_rows = tile_rows // 4
    tiles = PAIRS * GROUPS // 32
    r, c, d = lax.axis_index("row"), lax.axis_index("col"), lax.axis_index(DEPTH)
    place = jnp.stack([r, c, lax.axis_index(Z), lax.axis_index(Y)]).astype(jnp.int32)
    share = 32
    k_size = panels.shape[1]

    far = lax.ppermute(panels, "row", [(0, 1), (1, 0)])

    piece = shaped(z_size, tiles + 1, *TILE)
    parts = call(
        diag_kernel,
        "diag_part",
        8_000_000_000,
        [piece] * Y_SIZE,
        [SMEM, pl.BlockSpec((PB, k_size), lambda i: (i, 0))],
        [pltpu.VMEM((Y_SIZE, *piece.shape), F32)],
        grid=(2,),
        out_spec=pl.BlockSpec(piece.shape, lambda i: (0, 0, 0, 0)),
    )(place, panels)
    diag_sum = exchange(sum(delivered(parts, Y)), Z).sum(axis=0)

    a_sent = call(
        a_kernel,
        "a_pieces",
        1_000_000_000,
        [shaped(tiles + 1 + WIDE, *TILE)] * 4,
        [SMEM, ANY],
        [
            pltpu.VMEM((tiles, *TILE), F32),
            pltpu.VMEM((4, SUBLANES, PB), F32),
            pltpu.VMEM((32, LANES), F32),
            pltpu.SemaphoreType.DMA((tiles + 5,)),
        ],
    )(place, a_tile)
    a_got = sum(delivered(a_sent, "col"))

    difference = a_got[: tiles + 1] - diag_sum
    squares = jnp.sum(difference[tiles] * difference[tiles])
    diag_piece = jnp.concatenate([difference[:tiles], jnp.broadcast_to(squares, (1, *TILE))])
    other = lax.ppermute(diag_piece, "row", [(0, 1), (1, 0)])
    diag_piece = jnp.concatenate(
        [jnp.where(r == 0, diag_piece, other)[:tiles], (diag_piece + other)[tiles:]]
    )

    piece = shaped(z_size, WIDE, *TILE)
    parts = call(
        panel_kernel,
        "panel_part",
        4_000_000_000,
        [piece] * Y_SIZE,
        [SMEM, VMEM, ANY, ANY],
        [
            pltpu.VMEM((PB, k_size), F32),
            pltpu.VMEM((Y_SIZE, *piece.shape), F32),
            pltpu.SemaphoreType.DMA,
        ],
    )(place, lax.dynamic_slice_in_dim(panels, c * c_rows, c_rows, 0), panels, far)
    c_part = sum(delivered(parts, Y))

    got = exchange(
        jnp.concatenate([jnp.broadcast_to(diag_piece[None], (z_size, *diag_piece.shape)), c_part], axis=1), Z
    )
    diag_all = gathered(got[:, : tiles + 1], Y)
    c_piece = a_got[tiles + 1 :] - got[:, tiles + 1 :].sum(axis=0)

    piece = shaped(z_size, 4 * WIDE, *TILE)
    parts = call(
        block_kernel,
        "block_part",
        20_000_000_000,
        [piece] * Y_SIZE,
        [SMEM, pl.BlockSpec((LANES, k_size), lambda i: (i, 0)), ANY, ANY],
        [
            pltpu.VMEM((PB, k_size), jnp.bfloat16),
            pltpu.VMEM((PB, k_size), jnp.bfloat16),
            pltpu.VMEM((PB, k_size), F32),
            pltpu.SemaphoreType.DMA,
        ],
        grid=(z_size,),
        out_spec=pl.BlockSpec((1, *piece.shape[1:]), lambda i: (i, 0, 0, 0)),
    )(place, panels, panels, far)
    block = sum(delivered(parts, Y))

    got = exchange(
        jnp.concatenate([block, jnp.broadcast_to(c_piece[None], (z_size, *c_piece.shape))], axis=1), Z
    )
    block = got[:, : 4 * WIDE].sum(axis=0)
    block = block.reshape(4, WIDE, *TILE).transpose(0, 2, 1, 3).reshape(share, tile_cols)
    trailing = lax.dynamic_slice_in_dim(a_tile, d * share, share, 0) - block
    c_all = gathered(got[:, 4 * WIDE :], Y)

    inverse, norm = call(
        factor_kernel,
        "factor",
        30_000_000_000,
        [shaped(PB, PB), shaped(*TILE)],
        [SMEM] + [VMEM] * Y_SIZE,
        [pltpu.VMEM((PAIRS * LANES, LANES), F32), pltpu.VMEM((LANES, LANES), F32)],
    )(place, *diag_all)
    (new_panel,) = call(
        solve_kernel,
        "solve",
        2_000_000_000,
        [shaped(c_rows, PB)],
        [SMEM, VMEM] + [VMEM] * Y_SIZE,
        [pltpu.VMEM((c_rows, PB), F32)],
    )(place, inverse, *c_all)
    return (trailing, new_panel, norm[0, :1])


def solution(mesh):
    finer = Mesh(
        mesh.devices.reshape(mesh.shape["row"], mesh.shape["col"], 8, 4),
        ("row", "col", "depth_0", "depth_1"),
    )
    in_specs = (P("row", "col"), P("row", DEPTH))
    out_specs = (P(ROW_DEPTH, "col"), P(("row", "col"), None), P())
    return jax.shard_map(local, mesh=finer, in_specs=in_specs, out_specs=out_specs, check_vma=False)
```

```python
import jax
import jax.numpy as jnp
from jax import lax
from jax.experimental import pallas as pl
from jax.experimental.pallas import tpu as pltpu
from jax.sharding import Mesh
from jax.sharding import PartitionSpec as P


PB = 512
LANES = 128
SUBLANES = 8
GROUPS = LANES // SUBLANES
TILE = (SUBLANES, LANES)
BLOCKS = PB // LANES
PAIRS = BLOCKS * (BLOCKS + 1) // 2
DEPTH = ("depth_0", "depth_1")
ROW_DEPTH = ("row", "depth_0", "depth_1")
Z, Y = DEPTH
Y_SIZE = 4
WIDE = PB // LANES
F32 = jnp.float32


def times_transposed(left, right):
    return lax.dot_general(
        left,
        right,
        (((1,), (1,)), ((), ())),
        precision=lax.Precision.HIGHEST,
        preferred_element_type=F32,
    )


def pair(i, j):
    return i * (i + 1) // 2 + j


def inverse_factor(load, store):
    lane = lax.broadcasted_iota(jnp.int32, (SUBLANES, LANES), 1)
    sub = lax.broadcasted_iota(jnp.int32, (SUBLANES, LANES), 0)
    whole = (SUBLANES, LANES)
    rows = [load(h) for h in range(GROUPS)]
    for g in range(GROUPS):
        first = SUBLANES * g
        cols = {
            h: [
                jnp.broadcast_to(rows[h][:, first + j : first + j + 1], whole)
                for j in range(SUBLANES)
            ]
            for h in range(g, GROUPS)
        }
        inside = (lane >= first) & (lane < first + SUBLANES)
        rows[g] = jnp.where(inside, jnp.where(lane - first == sub, 1.0, 0.0), rows[g])
        for h in range(g + 1, GROUPS):
            rows[h] = jnp.where(inside, 0.0, rows[h])
        done = jnp.zeros(whole, F32)
        for j in range(SUBLANES):
            scale = lax.rsqrt(jnp.broadcast_to(cols[g][j][j : j + 1], whole))
            row = jnp.broadcast_to(rows[g][j : j + 1], whole) * scale
            done = jnp.where(sub == j, row, done)
            own = cols[g][j] * scale
            spread = {
                k: jnp.broadcast_to(own[k : k + 1], whole) for k in range(j + 1, SUBLANES)
            }
            for k in spread:
                cols[g][k] = cols[g][k] - own * spread[k]
            rows[g] = rows[g] - jnp.where(sub > j, own, 0.0) * row
            for h in range(g + 1, GROUPS):
                below = cols[h][j] * scale
                rows[h] = rows[h] - below * row
                for k in spread:
                    cols[h][k] = cols[h][k] - below * spread[k]
        store(g, jnp.where(lane <= first + sub, done, 0.0))


def halves(value):
    high = value.astype(jnp.bfloat16)
    return high, (value - high.astype(F32)).astype(jnp.bfloat16)


def product(left, right):
    def dot(a, b):
        return lax.dot_general(a, b, (((1,), (1,)), ((), ())), preferred_element_type=F32)

    return dot(left[0], right[0]) + (dot(left[0], right[1]) + dot(left[1], right[0]))


def diag_kernel(place_ref, p_ref, *refs):
    outs, all_ref = refs[:Y_SIZE], refs[Y_SIZE]
    step = pl.program_id(0)
    y = place_ref[3]
    lane = lax.broadcasted_iota(jnp.int32, TILE, 1)
    sub = lax.broadcasted_iota(jnp.int32, TILE, 0)
    per_piece = PAIRS * GROUPS // 32
    p = p_ref[...]
    squares = p * p
    folded = squares[:, :LANES]
    for l in range(1, p.shape[1] // LANES):
        folded = folded + squares[:, LANES * l : LANES * (l + 1)]
    ones = jnp.ones((SUBLANES, LANES), jnp.bfloat16)

    def row_sums(part):
        return lax.dot_general(ones, part, (((1,), (1,)), ((), ())), preferred_element_type=F32)

    high, low = halves(folded)
    sums = row_sums(high) + row_sums(low)
    for zz in range(WIDE):
        for yy in range(Y_SIZE):
            keep = (sub == 0) & (lane // 32 == yy)
            all_ref[yy, step * WIDE + zz, per_piece] = jnp.where(
                keep, sums[:, LANES * zz : LANES * (zz + 1)], 0.0
            )

    @pl.when(step == 0)
    def _():
        parts = halves(p)
        for i2 in range(BLOCKS // 2):
            wide = 2 * LANES * (i2 + 1)
            left = tuple(x[2 * LANES * i2 : 2 * LANES * (i2 + 1)] for x in parts)
            value = product(left, tuple(x[:wide] for x in parts))
            for i in (2 * i2, 2 * i2 + 1):
                for j in range(i + 1):
                    for h in range(GROUPS):
                        t = pair(i, j) * GROUPS + h
                        d, k = t // per_piece, t % per_piece
                        row = LANES * (i - 2 * i2) + SUBLANES * h
                        all_ref[d % Y_SIZE, d // Y_SIZE, k] = value[
                            row : row + SUBLANES, LANES * j : LANES * (j + 1)
                        ]

    @pl.when(step == 1)
    def _():
        for s in range(Y_SIZE):
            outs[s][...] = all_ref[lax.rem(y + s, Y_SIZE)]


def a_kernel(place_ref, a_ref, *refs):
    cols = 4
    outs = refs[:cols]
    tile_buf, panel_buf, own_buf, sem = refs[cols:]
    r, c, z, y = place_ref[0], place_ref[1], place_ref[2], place_ref[3]
    d = z * Y_SIZE + y
    per_piece = tile_buf.shape[0]
    copies = []
    for k in range(per_piece):
        t = d * per_piece + k
        b, h = t // GROUPS, lax.rem(t, GROUPS)
        i = (b >= 1).astype(jnp.int32) + (b >= 3).astype(jnp.int32) + (b >= 6).astype(jnp.int32)
        j = b - (i * (i + 1)) // 2
        row = pl.multiple_of(i * LANES + h * SUBLANES, SUBLANES)
        col = pl.multiple_of(j * LANES, LANES)
        copies.append((a_ref.at[pl.ds(row, SUBLANES), pl.ds(col, LANES)], tile_buf.at[k]))
    for s in range(cols):
        row = pl.multiple_of(lax.rem(c + s, cols) * 256 + d * SUBLANES, SUBLANES)
        copies.append((a_ref.at[pl.ds(row, SUBLANES), :], panel_buf.at[s]))
    row = pl.multiple_of(d * 32, 32)
    col = pl.multiple_of(lax.rem(z, WIDE) * LANES, LANES)
    copies.append((a_ref.at[pl.ds(row, 32), pl.ds(col, LANES)], own_buf))
    copies = [pltpu.make_async_copy(a, b, sem.at[n]) for n, (a, b) in enumerate(copies)]
    for copy in copies:
        copy.start()
    for copy in copies:
        copy.wait()
    lane = lax.broadcasted_iota(jnp.int32, (32, LANES), 1)
    sub = lax.broadcasted_iota(jnp.int32, (32, LANES), 0)
    diagonal = jnp.sum(jnp.where(lane == y * 32 + sub, own_buf[...], 0.0), axis=0, keepdims=True)
    holder = c == r * 2 + z // WIDE
    first = lax.broadcasted_iota(jnp.int32, TILE, 0) == 0
    diagonal = jnp.where(first & holder, jnp.broadcast_to(diagonal, TILE), 0.0)
    root = c == 0
    for s in range(cols):
        for k in range(per_piece):
            outs[s][k] = jnp.where(root, tile_buf[k], 0.0)
        outs[s][per_piece] = diagonal
        for l in range(WIDE):
            outs[s][per_piece + 1 + l] = jnp.where(
                root, panel_buf[s, :, LANES * l : LANES * (l + 1)], 0.0
            )


def panel_kernel(place_ref, near_ref, far_ref, *refs):
    outs, own_ref, top_ref, all_ref, sem = refs[:Y_SIZE], *refs[Y_SIZE:]
    r, c, y = place_ref[0], place_ref[1], place_ref[3]
    count = own_ref.shape[0]
    first = pl.multiple_of(c * count, count)
    own = pltpu.make_async_copy(near_ref.at[pl.ds(first, count)], own_ref, sem.at[0])
    own.start()

    @pl.when(r == 0)
    def _():
        pltpu.make_async_copy(near_ref.at[pl.ds(0, PB)], top_ref, sem.at[1]).start()

    @pl.when(r != 0)
    def _():
        pltpu.make_async_copy(far_ref.at[pl.ds(0, PB)], top_ref, sem.at[1]).start()

    own.wait()
    left = halves(own_ref[...])
    pltpu.make_async_copy(near_ref.at[pl.ds(0, PB)], top_ref, sem.at[1]).wait()
    value = product(left, halves(top_ref[...]))
    for g in range(count // SUBLANES):
        for l in range(WIDE):
            all_ref[g % Y_SIZE, g // Y_SIZE, l] = value[
                SUBLANES * g : SUBLANES * (g + 1), LANES * l : LANES * (l + 1)
            ]
    for s in range(Y_SIZE):
        outs[s][...] = all_ref[lax.rem(y + s, Y_SIZE)]


def block_kernel(place_ref, left_ref, near_ref, far_ref, *refs):
    outs, high_ref, low_ref, right_ref, sem = refs[:Y_SIZE], *refs[Y_SIZE:]
    r, c, y = place_ref[0], place_ref[1], place_ref[3]
    step = pl.program_id(0)
    here = c // 2 == r
    half = pl.multiple_of(lax.rem(c, 2) * PB, PB)

    @pl.when(step == 0)
    def _():
        @pl.when(here)
        def _():
            pltpu.make_async_copy(near_ref.at[pl.ds(half, PB)], right_ref, sem).start()

        @pl.when(jnp.logical_not(here))
        def _():
            pltpu.make_async_copy(far_ref.at[pl.ds(half, PB)], right_ref, sem).start()

        pltpu.make_async_copy(near_ref.at[pl.ds(half, PB)], right_ref, sem).wait()
        high, low = halves(right_ref[...])
        high_ref[...] = high
        low_ref[...] = low

    value = product(halves(left_ref[...]), (high_ref[...], low_ref[...]))
    for yy in range(Y_SIZE):
        for s in range(Y_SIZE):

            @pl.when(lax.rem(yy - y + Y_SIZE, Y_SIZE) == s)
            def _(yy=yy, s=s):
                for zz in range(outs[s].shape[0]):
                    for g in range(4):
                        for l in range(WIDE):
                            row = LANES * zz + 32 * yy + SUBLANES * g
                            outs[s][zz, g * WIDE + l] = value[
                                row : row + SUBLANES, LANES * l : LANES * (l + 1)
                            ]


def at(i, j):
    return slice(LANES * pair(i, j), LANES * (pair(i, j) + 1))


def block(i):
    return slice(LANES * i, LANES * (i + 1))


def factor_steps(steps, w, inv_ref, inverse_ref):
    def step(b, carry):
        start = (b * (b + 3)) // 2 * LANES

        def load(h):
            return w[pl.ds(pl.multiple_of(start + SUBLANES * h, SUBLANES), SUBLANES)]

        def store(h, value):
            inv_ref[SUBLANES * h : SUBLANES * (h + 1)] = value

        inverse_factor(load, store)
        for s in steps:

            @pl.when(b == s)
            def _(s=s):
                inv = inv_ref[...]
                for i in range(s + 1, BLOCKS):
                    w[at(i, s)] = times_transposed(w[at(i, s)], inv)
                for j in range(s + 1, BLOCKS):
                    for i in range(j, BLOCKS):
                        w[at(i, j)] = w[at(i, j)] - times_transposed(w[at(i, s)], w[at(j, s)])
                top = slice(0, LANES * (s + 1))
                x = times_transposed(inverse_ref[top, block(s)], inv)
                inverse_ref[top, block(s)] = x
                for j in range(s + 1, BLOCKS):
                    inverse_ref[top, block(j)] = inverse_ref[top, block(j)] - times_transposed(
                        x, w[at(j, s)]
                    )

        return carry

    lax.fori_loop(steps[0], steps[-1] + 1, step, 0)


def factor_first_kernel(place_ref, *refs):
    gathered, w, inverse_ref, norm_ref, inv_ref = refs[:Y_SIZE], *refs[Y_SIZE:]
    y = place_ref[3]
    z_size, per_piece = gathered[0].shape[0], gathered[0].shape[1] - 1
    total = jnp.zeros(TILE, F32)
    for s in range(Y_SIZE):
        source = lax.rem(y - s + Y_SIZE, Y_SIZE)
        for zz in range(z_size):
            for k in range(per_piece):
                t = (zz * Y_SIZE + source) * per_piece + k
                w[pl.ds(pl.multiple_of(t * SUBLANES, SUBLANES), SUBLANES)] = gathered[s][zz, k]
            total = total + gathered[s][zz, per_piece]
    norm_ref[...] = jnp.sqrt(total / 2048.0)
    lane = lax.broadcasted_iota(jnp.int32, (PB, PB), 1)
    sub = lax.broadcasted_iota(jnp.int32, (PB, PB), 0)
    inverse_ref[...] = jnp.where(lane == sub, 1.0, 0.0)
    factor_steps((0, 1), w, inv_ref, inverse_ref)


def factor_second_kernel(w_in_ref, inverse_in_ref, inverse_ref, w, inv_ref):
    for i in range(2, BLOCKS):
        for j in range(2, i + 1):
            w[at(i, j)] = w_in_ref[at(i, j)]
    inverse_ref[...] = inverse_in_ref[...]
    factor_steps((2, 3), w, inv_ref, inverse_ref)


def solve_kernel(place_ref, inverse_ref, *refs):
    gathered, x_ref, c_ref = refs[:Y_SIZE], *refs[Y_SIZE:]
    y = place_ref[3]
    for s in range(Y_SIZE):
        source = lax.rem(y - s + Y_SIZE, Y_SIZE)
        for zz in range(gathered[s].shape[0]):
            row = pl.multiple_of((zz * Y_SIZE + source) * SUBLANES, SUBLANES)
            for l in range(WIDE):
                c_ref[pl.ds(row, SUBLANES), LANES * l : LANES * (l + 1)] = gathered[s][zz, l]
    for l in range(WIDE):
        deep = slice(0, LANES * (l + 1))
        here = slice(LANES * l, LANES * (l + 1))
        x_ref[:, here] = jnp.dot(
            c_ref[:, deep],
            inverse_ref[deep, here],
            precision=lax.Precision.HIGHEST,
            preferred_element_type=F32,
        )


SMEM = pl.BlockSpec(memory_space=pltpu.SMEM)
VMEM = pl.BlockSpec(memory_space=pltpu.VMEM)
ANY = pl.BlockSpec(memory_space=pl.ANY)


def shaped(*dims):
    return jax.ShapeDtypeStruct(dims, F32)


def call(kernel, flops, outs, in_specs, scratch=(), grid=(), out_spec=None):
    out_specs = [out_spec or VMEM] * len(outs)
    return pl.pallas_call(
        kernel,
        out_shape=outs,
        grid=grid,
        in_specs=in_specs,
        out_specs=out_specs,
        scratch_shapes=scratch,
        cost_estimate=pl.CostEstimate(flops=flops, bytes_accessed=4_000_000, transcendentals=0),
    )


def exchange(pieces, axis):
    return lax.all_to_all(pieces, axis, split_axis=0, concat_axis=0, tiled=True)


def shifted(value, axis, by):
    size = lax.axis_size(axis)
    return lax.ppermute(value, axis, [(i, (i + by) % size) for i in range(size)])


def delivered(pieces, axis):
    return [pieces[0]] + [shifted(pieces[s], axis, s) for s in range(1, len(pieces))]


def gathered(value, axis):
    return delivered([value] * lax.axis_size(axis), axis)


def body(a_tile, panels):
    tile_rows, tile_cols = a_tile.shape
    z_size = lax.axis_size(Z)
    c_rows = tile_rows // 4
    tiles = PAIRS * GROUPS // 32
    r, c, d = lax.axis_index("row"), lax.axis_index("col"), lax.axis_index(DEPTH)
    place = jnp.stack([r, c, lax.axis_index(Z), lax.axis_index(Y)]).astype(jnp.int32)
    share = 32
    k_size = panels.shape[1]

    far = lax.ppermute(panels, "row", [(0, 1), (1, 0)])

    piece = shaped(z_size, tiles + 1, *TILE)
    parts = call(
        diag_kernel,
        8_000_000_000,
        [piece] * Y_SIZE,
        [SMEM, pl.BlockSpec((PB, k_size), lambda i: (i, 0))],
        [pltpu.VMEM((Y_SIZE, *piece.shape), F32)],
        grid=(2,),
        out_spec=pl.BlockSpec(piece.shape, lambda i: (0, 0, 0, 0)),
    )(place, panels)
    parts = delivered(parts, Y)
    part = sum(parts)
    diag_sum = exchange(part, Z)
    diag_sum = diag_sum.sum(axis=0)

    a_sent = call(
        a_kernel,
        1_000_000_000,
        [shaped(tiles + 1 + WIDE, *TILE)] * 4,
        [SMEM, ANY],
        [
            pltpu.VMEM((tiles, *TILE), F32),
            pltpu.VMEM((4, SUBLANES, PB), F32),
            pltpu.VMEM((32, LANES), F32),
            pltpu.SemaphoreType.DMA((tiles + 5,)),
        ],
    )(place, a_tile)
    a_got = delivered(a_sent, "col")
    a_got = sum(a_got)

    difference = a_got[: tiles + 1] - diag_sum
    squares = jnp.sum(difference[tiles] * difference[tiles])
    diag_piece = jnp.concatenate([difference[:tiles], jnp.broadcast_to(squares, (1, *TILE))])
    other = lax.ppermute(diag_piece, "row", [(0, 1), (1, 0)])
    diag_piece = jnp.concatenate(
        [jnp.where(r == 0, diag_piece, other)[:tiles], (diag_piece + other)[tiles:]]
    )

    piece = shaped(z_size, WIDE, *TILE)
    parts = call(
        panel_kernel,
        4_000_000_000,
        [piece] * Y_SIZE,
        [SMEM, ANY, ANY],
        [
            pltpu.VMEM((c_rows, k_size), F32),
            pltpu.VMEM((PB, k_size), F32),
            pltpu.VMEM((Y_SIZE, *piece.shape), F32),
            pltpu.SemaphoreType.DMA((2,)),
        ],
    )(place, panels, far)
    parts = delivered(parts, Y)
    c_part = sum(parts)

    sent = jnp.concatenate(
        [jnp.broadcast_to(diag_piece[None], (z_size, *diag_piece.shape)), c_part], axis=1
    )
    got = exchange(sent, Z)
    diag_all = gathered(got[:, : tiles + 1], Y)
    c_piece = a_got[tiles + 1 :] - got[:, tiles + 1 :].sum(axis=0)

    piece = shaped(z_size, 4 * WIDE, *TILE)
    parts = call(
        block_kernel,
        20_000_000_000,
        [piece] * Y_SIZE,
        [SMEM, pl.BlockSpec((PB, k_size), lambda i: (i, 0)), ANY, ANY],
        [
            pltpu.VMEM((PB, k_size), jnp.bfloat16),
            pltpu.VMEM((PB, k_size), jnp.bfloat16),
            pltpu.VMEM((PB, k_size), F32),
            pltpu.SemaphoreType.DMA,
        ],
        grid=(2,),
        out_spec=pl.BlockSpec((z_size // 2, *piece.shape[1:]), lambda i: (i, 0, 0, 0)),
    )(place, panels, panels, far)
    parts = delivered(parts, Y)
    block = sum(parts)

    sent = jnp.concatenate(
        [block, jnp.broadcast_to(c_piece[None], (z_size, *c_piece.shape))], axis=1
    )
    got = exchange(sent, Z)
    block = got[:, : 4 * WIDE].sum(axis=0)
    block = block.reshape(4, WIDE, *TILE).transpose(0, 2, 1, 3).reshape(share, tile_cols)
    trailing = lax.dynamic_slice_in_dim(a_tile, d * share, share, 0) - block
    c_all = gathered(got[:, 4 * WIDE :], Y)

    square = pltpu.VMEM((LANES, LANES), F32)
    w, inverse, norm = call(
        factor_first_kernel,
        15_000_000_000,
        [shaped(PAIRS * LANES, LANES), shaped(PB, PB), shaped(*TILE)],
        [SMEM] + [VMEM] * Y_SIZE,
        [square],
    )(place, *diag_all)
    (inverse,) = call(
        factor_second_kernel,
        15_000_000_000,
        [shaped(PB, PB)],
        [VMEM, VMEM],
        [pltpu.VMEM((PAIRS * LANES, LANES), F32), square],
    )(w, inverse)
    (new_panel,) = call(
        solve_kernel,
        2_000_000_000,
        [shaped(c_rows, PB)],
        [SMEM, VMEM] + [VMEM] * Y_SIZE,
        [pltpu.VMEM((c_rows, PB), F32)],
    )(place, inverse, *c_all)
    return (trailing, new_panel, norm[0, :1])


def solution(mesh):
    finer = Mesh(
        mesh.devices.reshape(mesh.shape["row"], mesh.shape["col"], 8, 4),
        ("row", "col", "depth_0", "depth_1"),
    )
    in_specs = (P("row", "col"), P("row", DEPTH))
    out_specs = (P(ROW_DEPTH, "col"), P(("row", "col"), None), P())
    return jax.shard_map(body, mesh=finer, in_specs=in_specs, out_specs=out_specs, check_vma=False)
```

```python
import jax
import jax.numpy as jnp
from jax import lax
from jax.experimental import pallas as pl
from jax.experimental.pallas import tpu as pltpu
from jax.sharding import Mesh
from jax.sharding import PartitionSpec as P


PB = 512
LANES = 128
SUBLANES = 8
GROUPS = LANES // SUBLANES
TILE = (SUBLANES, LANES)
BLOCKS = PB // LANES
PAIRS = BLOCKS * (BLOCKS + 1) // 2
DEPTH = ("depth_0", "depth_1")
ROW_DEPTH = ("row", "depth_0", "depth_1")
Z, Y = DEPTH
Y_SIZE = 4
WIDE = PB // LANES
SLOTS = 3
SUM_PIECE, SUM_SLOT = divmod(PAIRS * GROUPS // 2, SLOTS)
HALVES = (((0, 0), (3, 0), (3, 1), (3, 2), (3, 3)), ((1, 0), (1, 1), (2, 0), (2, 1), (2, 2)))
F32 = jnp.float32


def times_transposed(left, right):
    return lax.dot_general(
        left,
        right,
        (((1,), (1,)), ((), ())),
        precision=lax.Precision.HIGHEST,
        preferred_element_type=F32,
    )


def pair(i, j):
    return i * (i + 1) // 2 + j


def inverse_factor(load, store):
    lane = lax.broadcasted_iota(jnp.int32, (SUBLANES, LANES), 1)
    sub = lax.broadcasted_iota(jnp.int32, (SUBLANES, LANES), 0)
    whole = (SUBLANES, LANES)
    rows = [load(h) for h in range(GROUPS)]
    for g in range(GROUPS):
        first = SUBLANES * g
        cols = {
            h: [
                jnp.broadcast_to(rows[h][:, first + j : first + j + 1], whole)
                for j in range(SUBLANES)
            ]
            for h in range(g, GROUPS)
        }
        inside = (lane >= first) & (lane < first + SUBLANES)
        rows[g] = jnp.where(inside, jnp.where(lane - first == sub, 1.0, 0.0), rows[g])
        for h in range(g + 1, GROUPS):
            rows[h] = jnp.where(inside, 0.0, rows[h])
        done = jnp.zeros(whole, F32)
        for j in range(SUBLANES):
            scale = lax.rsqrt(jnp.broadcast_to(cols[g][j][j : j + 1], whole))
            row = jnp.broadcast_to(rows[g][j : j + 1], whole) * scale
            done = jnp.where(sub == j, row, done)
            own = cols[g][j] * scale
            spread = {
                k: jnp.broadcast_to(own[k : k + 1], whole) for k in range(j + 1, SUBLANES)
            }
            for k in spread:
                cols[g][k] = cols[g][k] - own * spread[k]
            rows[g] = rows[g] - jnp.where(sub > j, own, 0.0) * row
            for h in range(g + 1, GROUPS):
                below = cols[h][j] * scale
                rows[h] = rows[h] - below * row
                for k in spread:
                    cols[h][k] = cols[h][k] - below * spread[k]
        store(g, jnp.where(lane <= first + sub, done, 0.0))


def halves(value):
    high = value.astype(jnp.bfloat16)
    return high, (value - high.astype(F32)).astype(jnp.bfloat16)


def product(left, right):
    def dot(a, b):
        return lax.dot_general(a, b, (((1,), (1,)), ((), ())), preferred_element_type=F32)

    return dot(left[0], right[0]) + (dot(left[0], right[1]) + dot(left[1], right[0]))


def top_kernel(place_ref, near_ref, top_in_ref, out_ref, own_ref, top_ref, all_ref, sem):
    r, c = place_ref[0], place_ref[1]
    count = own_ref.shape[0]
    first = pl.multiple_of(c * count, count)
    own = pltpu.make_async_copy(near_ref.at[pl.ds(first, count)], own_ref, sem.at[0])
    every = pltpu.make_async_copy(near_ref, all_ref, sem.at[2])
    own.start()

    @pl.when(r == 0)
    def _():
        pltpu.make_async_copy(near_ref.at[pl.ds(0, PB)], top_ref, sem.at[1]).start()

    @pl.when(r != 0)
    def _():
        pltpu.make_async_copy(top_in_ref, top_ref, sem.at[1]).start()

    every.start()
    own.wait()
    pltpu.make_async_copy(top_in_ref, top_ref, sem.at[1]).wait()
    right = halves(top_ref[...])
    value = product(halves(own_ref[...]), right)
    for d in range(32):
        for l in range(WIDE):
            out_ref[d, SLOTS + l] = value[
                SUBLANES * d : SUBLANES * (d + 1), LANES * l : LANES * (l + 1)
            ]
    for half in range(2):

        @pl.when(r == half)
        def _(half=half):
            levels = sorted({i for i, _ in HALVES[half]})
            left = tuple(
                jnp.concatenate([x[LANES * i : LANES * (i + 1)] for i in levels]) for x in right
            )
            value = product(left, right)
            for b, (i, j) in enumerate(HALVES[half]):
                for h in range(GROUPS):
                    d, k = divmod(b * GROUPS + h, SLOTS)
                    row = LANES * levels.index(i) + SUBLANES * h
                    out_ref[d, k] = value[row : row + SUBLANES, LANES * j : LANES * (j + 1)]

    for t in range(PAIRS * GROUPS // 2 + 1, 32 * SLOTS):
        out_ref[t // SLOTS, t % SLOTS] = jnp.zeros(TILE, F32)
    every.wait()
    folded = jnp.zeros((all_ref.shape[0], LANES), F32)
    for l in range(all_ref.shape[1] // LANES):
        part = all_ref[:, LANES * l : LANES * (l + 1)]
        folded = folded + part * part
    ones = jnp.ones((SUBLANES, LANES), jnp.bfloat16)
    high, low = halves(folded)

    def row_sums(part):
        return lax.dot_general(ones, part, (((1,), (1,)), ((), ())), preferred_element_type=F32)

    sums = row_sums(high) + row_sums(low)
    sub = lax.broadcasted_iota(jnp.int32, TILE, 0)
    tile = jnp.zeros(TILE, F32)
    for a in range(SUBLANES):
        tile = jnp.where(sub == a, sums[:, LANES * a : LANES * (a + 1)], tile)
    out_ref[SUM_PIECE, SUM_SLOT] = tile


def a_kernel(place_ref, a_ref, *refs):
    cols = 4
    outs = refs[:cols]
    tile_buf, panel_buf, own_buf, sem = refs[cols:]
    r, c, d = place_ref[0], place_ref[1], place_ref[2] * Y_SIZE + place_ref[3]
    copies = []
    for k in range(SLOTS):
        t = jnp.minimum(d * SLOTS + k, PAIRS * GROUPS // 2 - 1)
        b, h = t // GROUPS, lax.rem(t, GROUPS)
        places = (
            (jnp.where(b == 0, 0, 3), jnp.where(b == 0, 0, b - 1)),
            (jnp.where(b < 2, 1, 2), jnp.where(b < 2, b, b - 2)),
        )
        for half, (i, j) in enumerate(places):
            row = pl.multiple_of(i * LANES + h * SUBLANES, SUBLANES)
            col = pl.multiple_of(j * LANES, LANES)
            copies.append(
                (a_ref.at[pl.ds(row, SUBLANES), pl.ds(col, LANES)], tile_buf.at[half * SLOTS + k])
            )
    for s in range(cols):
        row = pl.multiple_of(lax.rem(c + s, cols) * 256 + d * SUBLANES, SUBLANES)
        copies.append((a_ref.at[pl.ds(row, SUBLANES), :], panel_buf.at[s]))
    for b in range(BLOCKS):
        row = pl.multiple_of(lax.rem(c, 2) * PB + b * LANES, LANES)
        copies.append((a_ref.at[pl.ds(row, LANES), pl.ds(b * LANES, LANES)], own_buf.at[b]))
    copies = [pltpu.make_async_copy(a, b, sem.at[n]) for n, (a, b) in enumerate(copies)]
    for copy in copies:
        copy.start()
    for copy in copies:
        copy.wait()
    lane = lax.broadcasted_iota(jnp.int32, (LANES, LANES), 1)
    sub = lax.broadcasted_iota(jnp.int32, (LANES, LANES), 0)
    level = lax.broadcasted_iota(jnp.int32, TILE, 0)
    diagonal = jnp.zeros(TILE, F32)
    for b in range(BLOCKS):
        values = jnp.sum(jnp.where(lane == sub, own_buf[b], 0.0), axis=0, keepdims=True)
        here = (level == lax.rem(c, 2) * BLOCKS + b) & (c // 2 == r)
        diagonal = jnp.where(here, jnp.broadcast_to(values, TILE), diagonal)
    root = c == 0
    for s in range(cols):
        for k in range(2 * SLOTS):
            outs[s][k] = jnp.where(root, tile_buf[k], 0.0)
        for l in range(WIDE):
            outs[s][2 * SLOTS + l] = jnp.where(
                root, panel_buf[s, :, LANES * l : LANES * (l + 1)], 0.0
            )
        outs[s][2 * SLOTS + WIDE] = diagonal


def merge_kernel(place_ref, got_ref, a_ref, other_ref, out_ref):
    r, d = place_ref[0], place_ref[2] * Y_SIZE + place_ref[3]
    total = got_ref[0]
    for n in range(1, got_ref.shape[0]):
        total = total + got_ref[n]
    tiles = []
    for k in range(SLOTS):
        a = jnp.where(r == 0, a_ref[k], other_ref[k])
        if k == SUM_SLOT:
            special = d == SUM_PIECE
            value = jnp.where(special, a_ref[2 * SLOTS + WIDE], a) - total[k]
            squares = jnp.sum(jnp.sum(value * value, axis=1, keepdims=True), axis=0, keepdims=True)
            tiles.append(jnp.where(special, jnp.broadcast_to(squares, TILE), value))
        else:
            tiles.append(a - total[k])
    for l in range(WIDE):
        tiles.append(a_ref[2 * SLOTS + l] - total[SLOTS + l])
    for n in range(out_ref.shape[0]):
        for k, tile in enumerate(tiles):
            out_ref[n, k] = tile


def block_kernel(place_ref, left_ref, near_ref, far_ref, *refs):
    outs, high_ref, low_ref, right_ref, sem = refs[:Y_SIZE], *refs[Y_SIZE:]
    r, c, y = place_ref[0], place_ref[1], place_ref[3]
    step = pl.program_id(0)
    here = c // 2 == r
    half = pl.multiple_of(lax.rem(c, 2) * PB, PB)

    @pl.when(step == 0)
    def _():
        @pl.when(here)
        def _():
            pltpu.make_async_copy(near_ref.at[pl.ds(half, PB)], right_ref, sem).start()

        @pl.when(jnp.logical_not(here))
        def _():
            pltpu.make_async_copy(far_ref.at[pl.ds(half, PB)], right_ref, sem).start()

        pltpu.make_async_copy(near_ref.at[pl.ds(half, PB)], right_ref, sem).wait()
        high, low = halves(right_ref[...])
        high_ref[...] = high
        low_ref[...] = low

    value = product(halves(left_ref[...]), (high_ref[...], low_ref[...]))
    for yy in range(Y_SIZE):
        for s in range(Y_SIZE):

            @pl.when(lax.rem(yy - y + Y_SIZE, Y_SIZE) == s)
            def _(yy=yy, s=s):
                for zz in range(outs[s].shape[0]):
                    for g in range(4):
                        for l in range(WIDE):
                            row = LANES * zz + 32 * yy + SUBLANES * g
                            outs[s][zz, g * WIDE + l] = value[
                                row : row + SUBLANES, LANES * l : LANES * (l + 1)
                            ]


def at(i, j):
    return slice(LANES * pair(i, j), LANES * (pair(i, j) + 1))


def block(i):
    return slice(LANES * i, LANES * (i + 1))


def solve_kernel(place_ref, mine_ref, other_ref, x_ref, norm_ref, w, inv_ref):
    r = place_ref[0]
    for half in range(2):
        for ref, take in ((mine_ref, r == half), (other_ref, r != half)):

            @pl.when(take)
            def _(half=half, ref=ref):
                for b, (i, j) in enumerate(HALVES[half]):
                    for h in range(GROUPS):
                        d, k = divmod(b * GROUPS + h, SLOTS)
                        row = LANES * pair(i, j) + SUBLANES * h
                        w[row : row + SUBLANES] = ref[d, k]

    for d in range(mine_ref.shape[0]):
        for l in range(WIDE):
            x_ref[SUBLANES * d : SUBLANES * (d + 1), block(l)] = mine_ref[d, SLOTS + l]
    total = mine_ref[SUM_PIECE, SUM_SLOT] + other_ref[SUM_PIECE, SUM_SLOT]
    norm_ref[...] = jnp.sqrt(total / 2048.0)

    def step(b, carry):
        start = (b * (b + 3)) // 2 * LANES

        def load(h):
            return w[pl.ds(pl.multiple_of(start + SUBLANES * h, SUBLANES), SUBLANES)]

        def store(h, value):
            inv_ref[SUBLANES * h : SUBLANES * (h + 1)] = value

        inverse_factor(load, store)
        for s in range(BLOCKS):

            @pl.when(b == s)
            def _(s=s):
                inv = inv_ref[...]
                for i in range(s + 1, BLOCKS):
                    w[at(i, s)] = times_transposed(w[at(i, s)], inv)
                for j in range(s + 1, BLOCKS):
                    for i in range(j, BLOCKS):
                        w[at(i, j)] = w[at(i, j)] - times_transposed(w[at(i, s)], w[at(j, s)])
                x = times_transposed(x_ref[:, block(s)], inv)
                x_ref[:, block(s)] = x
                for j in range(s + 1, BLOCKS):
                    x_ref[:, block(j)] = x_ref[:, block(j)] - times_transposed(x, w[at(j, s)])

        return carry

    lax.fori_loop(0, BLOCKS, step, 0)


SMEM = pl.BlockSpec(memory_space=pltpu.SMEM)
VMEM = pl.BlockSpec(memory_space=pltpu.VMEM)
ANY = pl.BlockSpec(memory_space=pl.ANY)


def shaped(*dims):
    return jax.ShapeDtypeStruct(dims, F32)


def call(kernel, flops, outs, in_specs, scratch=(), grid=(), out_spec=None):
    out_specs = [out_spec or VMEM] * len(outs)
    return pl.pallas_call(
        kernel,
        out_shape=outs,
        grid=grid,
        in_specs=in_specs,
        out_specs=out_specs,
        scratch_shapes=scratch,
        cost_estimate=pl.CostEstimate(flops=flops, bytes_accessed=4_000_000, transcendentals=0),
    )


def exchange(pieces, axis):
    return lax.all_to_all(pieces, axis, split_axis=0, concat_axis=0, tiled=True)


def shifted(value, axis, by):
    size = lax.axis_size(axis)
    return lax.ppermute(value, axis, [(i, (i + by) % size) for i in range(size)])


def delivered(pieces, axis):
    return [pieces[0]] + [shifted(pieces[s], axis, s) for s in range(1, len(pieces))]


def body(a_tile, panels):
    tile_rows, tile_cols = a_tile.shape
    z_size, depth = lax.axis_size(Z), lax.axis_size(DEPTH)
    c_rows = tile_rows // 4
    share = tile_rows // depth
    k_size = panels.shape[1]
    r, c, d = lax.axis_index("row"), lax.axis_index("col"), lax.axis_index(DEPTH)
    place = jnp.stack([r, c, lax.axis_index(Z), lax.axis_index(Y)]).astype(jnp.int32)
    swap = [(0, 1), (1, 0)]

    top = lax.ppermute(panels[:PB], "row", [(0, 1)])
    far = lax.ppermute(panels, "row", swap)

    piece = shaped(depth, SLOTS + WIDE, *TILE)
    (part,) = call(
        top_kernel,
        8_000_000_000,
        [piece],
        [SMEM, ANY, ANY],
        [
            pltpu.VMEM((c_rows, k_size), F32),
            pltpu.VMEM((PB, k_size), F32),
            pltpu.VMEM((tile_rows, k_size), F32),
            pltpu.SemaphoreType.DMA((3,)),
        ],
    )(place, panels, top)
    got = exchange(part, DEPTH)

    a_sent = call(
        a_kernel,
        1_000_000_000,
        [shaped(2 * SLOTS + WIDE + 1, *TILE)] * 4,
        [SMEM, ANY],
        [
            pltpu.VMEM((2 * SLOTS, *TILE), F32),
            pltpu.VMEM((4, SUBLANES, PB), F32),
            pltpu.VMEM((BLOCKS, LANES, LANES), F32),
            pltpu.SemaphoreType.DMA((2 * SLOTS + 4 + BLOCKS,)),
        ],
    )(place, a_tile)
    a_got = delivered(a_sent, "col")
    a_got = sum(a_got)
    a_other = lax.ppermute(a_got[SLOTS : 2 * SLOTS], "row", [(0, 1)])

    (piece_copies,) = call(
        merge_kernel, 1_000_000_000, [piece], [SMEM, VMEM, VMEM, VMEM]
    )(place, got, a_got, a_other)
    mine = exchange(piece_copies, DEPTH)
    other = lax.ppermute(mine[:, :SLOTS], "row", swap)

    piece = shaped(z_size, 4 * WIDE, *TILE)
    parts = call(
        block_kernel,
        20_000_000_000,
        [piece] * Y_SIZE,
        [SMEM, pl.BlockSpec((PB, k_size), lambda i: (i, 0)), ANY, ANY],
        [
            pltpu.VMEM((PB, k_size), jnp.bfloat16),
            pltpu.VMEM((PB, k_size), jnp.bfloat16),
            pltpu.VMEM((PB, k_size), F32),
            pltpu.SemaphoreType.DMA,
        ],
        grid=(2,),
        out_spec=pl.BlockSpec((z_size // 2, *piece.shape[1:]), lambda i: (i, 0, 0, 0)),
    )(place, panels, panels, far)
    parts = delivered(parts, Y)
    part = sum(parts)
    got = exchange(part, Z)
    tiles = got.sum(axis=0)
    tiles = tiles.reshape(4, WIDE, *TILE).transpose(0, 2, 1, 3).reshape(share, tile_cols)
    trailing = lax.dynamic_slice_in_dim(a_tile, d * share, share, 0) - tiles

    new_panel, norm = call(
        solve_kernel,
        30_000_000_000,
        [shaped(c_rows, PB), shaped(*TILE)],
        [SMEM, VMEM, VMEM],
        [pltpu.VMEM((PAIRS * LANES, LANES), F32), pltpu.VMEM((LANES, LANES), F32)],
    )(place, mine, other)
    return (trailing, new_panel, norm[0, :1])


def solution(mesh):
    finer = Mesh(
        mesh.devices.reshape(mesh.shape["row"], mesh.shape["col"], 8, 4),
        ("row", "col", "depth_0", "depth_1"),
    )
    in_specs = (P("row", "col"), P("row", DEPTH))
    out_specs = (P(ROW_DEPTH, "col"), P(("row", "col"), None), P())
    return jax.shard_map(body, mesh=finer, in_specs=in_specs, out_specs=out_specs, check_vma=False)
```

```python
import jax
import jax.numpy as jnp
from jax import lax
from jax.experimental import pallas as pl
from jax.experimental.pallas import tpu as pltpu
from jax.sharding import Mesh
from jax.sharding import PartitionSpec as P


PB = 512
LANES = 128
SUBLANES = 8
GROUPS = LANES // SUBLANES
TILE = (SUBLANES, LANES)
BLOCKS = PB // LANES
PAIRS = BLOCKS * (BLOCKS + 1) // 2
DEPTH = ("depth_0", "depth_1")
ROW_DEPTH = ("row", "depth_0", "depth_1")
Z, Y = DEPTH
Y_SIZE = 4
WIDE = PB // LANES
SLOTS = 3
SUM_PIECE, SUM_SLOT = divmod(PAIRS * GROUPS // 2, SLOTS)
HALVES = (((0, 0), (3, 0), (3, 1), (3, 2), (3, 3)), ((1, 0), (1, 1), (2, 0), (2, 1), (2, 2)))
F32 = jnp.float32


def times_transposed(left, right):
    return lax.dot_general(
        left,
        right,
        (((1,), (1,)), ((), ())),
        precision=lax.Precision.HIGHEST,
        preferred_element_type=F32,
    )


def pair(i, j):
    return i * (i + 1) // 2 + j


def inverse_factor(load, store):
    lane = lax.broadcasted_iota(jnp.int32, (SUBLANES, LANES), 1)
    sub = lax.broadcasted_iota(jnp.int32, (SUBLANES, LANES), 0)
    whole = (SUBLANES, LANES)
    rows = [load(h) for h in range(GROUPS)]
    for g in range(GROUPS):
        first = SUBLANES * g
        cols = {
            h: [
                jnp.broadcast_to(rows[h][:, first + j : first + j + 1], whole)
                for j in range(SUBLANES)
            ]
            for h in range(g, GROUPS)
        }
        inside = (lane >= first) & (lane < first + SUBLANES)
        rows[g] = jnp.where(inside, jnp.where(lane - first == sub, 1.0, 0.0), rows[g])
        for h in range(g + 1, GROUPS):
            rows[h] = jnp.where(inside, 0.0, rows[h])
        done = jnp.zeros(whole, F32)
        for j in range(SUBLANES):
            scale = lax.rsqrt(jnp.broadcast_to(cols[g][j][j : j + 1], whole))
            row = jnp.broadcast_to(rows[g][j : j + 1], whole) * scale
            done = jnp.where(sub == j, row, done)
            own = cols[g][j] * scale
            spread = {
                k: jnp.broadcast_to(own[k : k + 1], whole) for k in range(j + 1, SUBLANES)
            }
            for k in spread:
                cols[g][k] = cols[g][k] - own * spread[k]
            rows[g] = rows[g] - jnp.where(sub > j, own, 0.0) * row
            for h in range(g + 1, GROUPS):
                below = cols[h][j] * scale
                rows[h] = rows[h] - below * row
                for k in spread:
                    cols[h][k] = cols[h][k] - below * spread[k]
        store(g, jnp.where(lane <= first + sub, done, 0.0))


def halves(value):
    high = value.astype(jnp.bfloat16)
    return high, (value - high.astype(F32)).astype(jnp.bfloat16)


def product(left, right):
    def dot(a, b):
        return lax.dot_general(a, b, (((1,), (1,)), ((), ())), preferred_element_type=F32)

    return dot(left[0], right[0]) + (dot(left[0], right[1]) + dot(left[1], right[0]))


def top_kernel(place_ref, near_ref, top_in_ref, out_ref, own_ref, top_ref, all_ref, sem):
    r, c = place_ref[0], place_ref[1]
    count = own_ref.shape[0]
    first = pl.multiple_of(c * count, count)
    own = pltpu.make_async_copy(near_ref.at[pl.ds(first, count)], own_ref, sem.at[0])
    every = pltpu.make_async_copy(near_ref, all_ref, sem.at[2])
    own.start()

    @pl.when(r == 0)
    def _():
        pltpu.make_async_copy(near_ref.at[pl.ds(0, PB)], top_ref, sem.at[1]).start()

    @pl.when(r != 0)
    def _():
        pltpu.make_async_copy(top_in_ref, top_ref, sem.at[1]).start()

    every.start()
    own.wait()
    pltpu.make_async_copy(top_in_ref, top_ref, sem.at[1]).wait()
    right = halves(top_ref[...])
    value = product(halves(own_ref[...]), right)
    for d in range(32):
        for l in range(WIDE):
            out_ref[d, SLOTS + l] = value[
                SUBLANES * d : SUBLANES * (d + 1), LANES * l : LANES * (l + 1)
            ]
    for half in range(2):

        @pl.when(r == half)
        def _(half=half):
            levels = sorted({i for i, _ in HALVES[half]})
            left = tuple(
                jnp.concatenate([x[LANES * i : LANES * (i + 1)] for i in levels]) for x in right
            )
            value = product(left, right)
            for b, (i, j) in enumerate(HALVES[half]):
                for h in range(GROUPS):
                    d, k = divmod(b * GROUPS + h, SLOTS)
                    row = LANES * levels.index(i) + SUBLANES * h
                    out_ref[d, k] = value[row : row + SUBLANES, LANES * j : LANES * (j + 1)]

    for t in range(PAIRS * GROUPS // 2 + 1, 32 * SLOTS):
        out_ref[t // SLOTS, t % SLOTS] = jnp.zeros(TILE, F32)
    every.wait()
    folded = jnp.zeros((all_ref.shape[0], LANES), F32)
    for l in range(all_ref.shape[1] // LANES):
        part = all_ref[:, LANES * l : LANES * (l + 1)]
        folded = folded + part * part
    ones = jnp.ones((SUBLANES, LANES), jnp.bfloat16)
    high, low = halves(folded)

    def row_sums(part):
        return lax.dot_general(ones, part, (((1,), (1,)), ((), ())), preferred_element_type=F32)

    sums = row_sums(high) + row_sums(low)
    sub = lax.broadcasted_iota(jnp.int32, TILE, 0)
    tile = jnp.zeros(TILE, F32)
    for a in range(SUBLANES):
        tile = jnp.where(sub == a, sums[:, LANES * a : LANES * (a + 1)], tile)
    out_ref[SUM_PIECE, SUM_SLOT] = tile


def a_kernel(place_ref, a_ref, *refs):
    cols = 4
    outs = refs[:cols]
    tile_buf, panel_buf, own_buf, sem = refs[cols:]
    r, c, d = place_ref[0], place_ref[1], place_ref[2] * Y_SIZE + place_ref[3]
    copies = []
    for k in range(SLOTS):
        t = jnp.minimum(d * SLOTS + k, PAIRS * GROUPS // 2 - 1)
        b, h = t // GROUPS, lax.rem(t, GROUPS)
        places = (
            (jnp.where(b == 0, 0, 3), jnp.where(b == 0, 0, b - 1)),
            (jnp.where(b < 2, 1, 2), jnp.where(b < 2, b, b - 2)),
        )
        for half, (i, j) in enumerate(places):
            row = pl.multiple_of(i * LANES + h * SUBLANES, SUBLANES)
            col = pl.multiple_of(j * LANES, LANES)
            copies.append(
                (a_ref.at[pl.ds(row, SUBLANES), pl.ds(col, LANES)], tile_buf.at[half * SLOTS + k])
            )
    for s in range(cols):
        row = pl.multiple_of(lax.rem(c + s, cols) * 256 + d * SUBLANES, SUBLANES)
        copies.append((a_ref.at[pl.ds(row, SUBLANES), :], panel_buf.at[s]))
    for b in range(BLOCKS):
        row = pl.multiple_of(lax.rem(c, 2) * PB + b * LANES, LANES)
        copies.append((a_ref.at[pl.ds(row, LANES), pl.ds(b * LANES, LANES)], own_buf.at[b]))
    copies = [pltpu.make_async_copy(a, b, sem.at[n]) for n, (a, b) in enumerate(copies)]
    for copy in copies:
        copy.start()
    for copy in copies:
        copy.wait()
    lane = lax.broadcasted_iota(jnp.int32, (LANES, LANES), 1)
    sub = lax.broadcasted_iota(jnp.int32, (LANES, LANES), 0)
    level = lax.broadcasted_iota(jnp.int32, TILE, 0)
    diagonal = jnp.zeros(TILE, F32)
    for b in range(BLOCKS):
        values = jnp.sum(jnp.where(lane == sub, own_buf[b], 0.0), axis=0, keepdims=True)
        here = (level == lax.rem(c, 2) * BLOCKS + b) & (c // 2 == r)
        diagonal = jnp.where(here, jnp.broadcast_to(values, TILE), diagonal)
    root = c == 0
    for s in range(cols):
        for k in range(2 * SLOTS):
            outs[s][k] = jnp.where(root, tile_buf[k], 0.0)
        for l in range(WIDE):
            outs[s][2 * SLOTS + l] = jnp.where(
                root, panel_buf[s, :, LANES * l : LANES * (l + 1)], 0.0
            )
        outs[s][2 * SLOTS + WIDE] = diagonal


def merge_kernel(place_ref, got_ref, a_ref, other_ref, out_ref):
    r, d = place_ref[0], place_ref[2] * Y_SIZE + place_ref[3]
    total = got_ref[0]
    for n in range(1, got_ref.shape[0]):
        total = total + got_ref[n]
    tiles = []
    for k in range(SLOTS):
        a = jnp.where(r == 0, a_ref[k], other_ref[k])
        if k == SUM_SLOT:
            special = d == SUM_PIECE
            value = jnp.where(special, a_ref[2 * SLOTS + WIDE], a) - total[k]
            squares = jnp.sum(jnp.sum(value * value, axis=1, keepdims=True), axis=0, keepdims=True)
            tiles.append(jnp.where(special, jnp.broadcast_to(squares, TILE), value))
        else:
            tiles.append(a - total[k])
    for l in range(WIDE):
        tiles.append(a_ref[2 * SLOTS + l] - total[SLOTS + l])
    for n in range(out_ref.shape[0]):
        for k, tile in enumerate(tiles):
            out_ref[n, k] = tile


def block_kernel(place_ref, left_ref, near_ref, far_ref, *refs):
    outs, high_ref, low_ref, right_ref, sem = refs[:Y_SIZE], *refs[Y_SIZE:]
    r, c, y = place_ref[0], place_ref[1], place_ref[3]
    step = pl.program_id(0)
    here = c // 2 == r
    half = pl.multiple_of(lax.rem(c, 2) * PB, PB)

    @pl.when(step == 0)
    def _():
        @pl.when(here)
        def _():
            pltpu.make_async_copy(near_ref.at[pl.ds(half, PB)], right_ref, sem).start()

        @pl.when(jnp.logical_not(here))
        def _():
            pltpu.make_async_copy(far_ref.at[pl.ds(half, PB)], right_ref, sem).start()

        pltpu.make_async_copy(near_ref.at[pl.ds(half, PB)], right_ref, sem).wait()
        high, low = halves(right_ref[...])
        high_ref[...] = high
        low_ref[...] = low

    value = product(halves(left_ref[...]), (high_ref[...], low_ref[...]))
    for yy in range(Y_SIZE):
        for s in range(Y_SIZE):

            @pl.when(lax.rem(yy - y + Y_SIZE, Y_SIZE) == s)
            def _(yy=yy, s=s):
                for zz in range(outs[s].shape[0]):
                    for g in range(4):
                        for l in range(WIDE):
                            row = LANES * zz + 32 * yy + SUBLANES * g
                            outs[s][zz, g * WIDE + l] = value[
                                row : row + SUBLANES, LANES * l : LANES * (l + 1)
                            ]


def at(i, j):
    return slice(LANES * pair(i, j), LANES * (pair(i, j) + 1))


def block(i):
    return slice(LANES * i, LANES * (i + 1))


def solve_kernel(place_ref, mine_ref, other_ref, x_ref, norm_ref, w):
    r = place_ref[0]
    for half in range(2):
        for ref, take in ((mine_ref, r == half), (other_ref, r != half)):

            @pl.when(take)
            def _(half=half, ref=ref):
                for b, (i, j) in enumerate(HALVES[half]):
                    for h in range(GROUPS):
                        d, k = divmod(b * GROUPS + h, SLOTS)
                        row = LANES * pair(i, j) + SUBLANES * h
                        w[row : row + SUBLANES] = ref[d, k]

    for d in range(mine_ref.shape[0]):
        for l in range(WIDE):
            x_ref[SUBLANES * d : SUBLANES * (d + 1), block(l)] = mine_ref[d, SLOTS + l]
    total = mine_ref[SUM_PIECE, SUM_SLOT] + other_ref[SUM_PIECE, SUM_SLOT]
    norm_ref[...] = jnp.sqrt(total / 2048.0)

    low = {(i, j): w[at(i, j)] for i in range(BLOCKS) for j in range(i + 1)}
    rows = [x_ref[:, block(l)] for l in range(WIDE)]
    for s in range(BLOCKS):
        parts = [None] * GROUPS

        def load(h, square=low[s, s]):
            return square[SUBLANES * h : SUBLANES * (h + 1)]

        inverse_factor(load, parts.__setitem__)
        inv = jnp.concatenate(parts)
        for i in range(s + 1, BLOCKS):
            low[i, s] = times_transposed(low[i, s], inv)
        for j in range(s + 1, BLOCKS):
            for i in range(j, BLOCKS):
                low[i, j] = low[i, j] - times_transposed(low[i, s], low[j, s])
        x = times_transposed(rows[s], inv)
        x_ref[:, block(s)] = x
        for j in range(s + 1, BLOCKS):
            rows[j] = rows[j] - times_transposed(x, low[j, s])


def trailing_kernel(place_ref, got_ref, a_ref, out_ref, a_buf, sem):
    share = out_ref.shape[0]
    row = pl.multiple_of((place_ref[2] * Y_SIZE + place_ref[3]) * share, share)
    copy = pltpu.make_async_copy(a_ref.at[pl.ds(row, share)], a_buf, sem)
    copy.start()
    copy.wait()
    for g in range(share // SUBLANES):
        for l in range(WIDE):
            total = got_ref[0, g * WIDE + l]
            for n in range(1, got_ref.shape[0]):
                total = total + got_ref[n, g * WIDE + l]
            here = (slice(SUBLANES * g, SUBLANES * (g + 1)), slice(LANES * l, LANES * (l + 1)))
            out_ref[here] = a_buf[here] - total


SMEM = pl.BlockSpec(memory_space=pltpu.SMEM)
VMEM = pl.BlockSpec(memory_space=pltpu.VMEM)
ANY = pl.BlockSpec(memory_space=pl.ANY)


def shaped(*dims):
    return jax.ShapeDtypeStruct(dims, F32)


def call(kernel, flops, outs, in_specs, scratch=(), grid=(), out_spec=None):
    out_specs = [out_spec or VMEM] * len(outs)
    return pl.pallas_call(
        kernel,
        out_shape=outs,
        grid=grid,
        in_specs=in_specs,
        out_specs=out_specs,
        scratch_shapes=scratch,
        cost_estimate=pl.CostEstimate(flops=flops, bytes_accessed=4_000_000, transcendentals=0),
    )


def exchange(pieces, axis):
    return lax.all_to_all(pieces, axis, split_axis=0, concat_axis=0, tiled=True)


def shifted(value, axis, by):
    size = lax.axis_size(axis)
    return lax.ppermute(value, axis, [(i, (i + by) % size) for i in range(size)])


def delivered(pieces, axis):
    return [pieces[0]] + [shifted(pieces[s], axis, s) for s in range(1, len(pieces))]


def body(a_tile, panels):
    tile_rows, tile_cols = a_tile.shape
    z_size, depth = lax.axis_size(Z), lax.axis_size(DEPTH)
    c_rows = tile_rows // 4
    share = tile_rows // depth
    k_size = panels.shape[1]
    r, c = lax.axis_index("row"), lax.axis_index("col")
    place = jnp.stack([r, c, lax.axis_index(Z), lax.axis_index(Y)]).astype(jnp.int32)
    swap = [(0, 1), (1, 0)]

    top = lax.ppermute(panels[:PB], "row", [(0, 1)])
    far = lax.ppermute(panels, "row", swap)

    piece = shaped(depth, SLOTS + WIDE, *TILE)
    (part,) = call(
        top_kernel,
        8_000_000_000,
        [piece],
        [SMEM, ANY, ANY],
        [
            pltpu.VMEM((c_rows, k_size), F32),
            pltpu.VMEM((PB, k_size), F32),
            pltpu.VMEM((tile_rows, k_size), F32),
            pltpu.SemaphoreType.DMA((3,)),
        ],
    )(place, panels, top)
    got = exchange(part, DEPTH)

    a_sent = call(
        a_kernel,
        1_000_000_000,
        [shaped(2 * SLOTS + WIDE + 1, *TILE)] * 4,
        [SMEM, ANY],
        [
            pltpu.VMEM((2 * SLOTS, *TILE), F32),
            pltpu.VMEM((4, SUBLANES, PB), F32),
            pltpu.VMEM((BLOCKS, LANES, LANES), F32),
            pltpu.SemaphoreType.DMA((2 * SLOTS + 4 + BLOCKS,)),
        ],
    )(place, a_tile)
    a_got = delivered(a_sent, "col")
    a_got = sum(a_got)
    a_other = lax.ppermute(a_got[SLOTS : 2 * SLOTS], "row", [(0, 1)])

    (piece_copies,) = call(
        merge_kernel, 1_000_000_000, [piece], [SMEM, VMEM, VMEM, VMEM]
    )(place, got, a_got, a_other)
    mine = exchange(piece_copies, DEPTH)
    other = lax.ppermute(mine[:, :SLOTS], "row", swap)

    piece = shaped(z_size, 4 * WIDE, *TILE)
    parts = call(
        block_kernel,
        20_000_000_000,
        [piece] * Y_SIZE,
        [SMEM, pl.BlockSpec((PB, k_size), lambda i: (i, 0)), ANY, ANY],
        [
            pltpu.VMEM((PB, k_size), jnp.bfloat16),
            pltpu.VMEM((PB, k_size), jnp.bfloat16),
            pltpu.VMEM((PB, k_size), F32),
            pltpu.SemaphoreType.DMA,
        ],
        grid=(2,),
        out_spec=pl.BlockSpec((z_size // 2, *piece.shape[1:]), lambda i: (i, 0, 0, 0)),
    )(place, panels, panels, far)
    parts = delivered(parts, Y)
    part = sum(parts)
    got = exchange(part, Z)
    (trailing,) = call(
        trailing_kernel,
        1_000_000_000,
        [shaped(share, tile_cols)],
        [SMEM, VMEM, ANY],
        [pltpu.VMEM((share, tile_cols), F32), pltpu.SemaphoreType.DMA],
    )(place, got, a_tile)

    new_panel, norm = call(
        solve_kernel,
        30_000_000_000,
        [shaped(c_rows, PB), shaped(*TILE)],
        [SMEM, VMEM, VMEM],
        [pltpu.VMEM((PAIRS * LANES, LANES), F32)],
    )(place, mine, other)
    return (trailing, new_panel, norm[0, :1])


def solution(mesh):
    finer = Mesh(
        mesh.devices.reshape(mesh.shape["row"], mesh.shape["col"], 8, 4),
        ("row", "col", "depth_0", "depth_1"),
    )
    in_specs = (P("row", "col"), P("row", DEPTH))
    out_specs = (P(ROW_DEPTH, "col"), P(("row", "col"), None), P())
    return jax.shard_map(body, mesh=finer, in_specs=in_specs, out_specs=out_specs, check_vma=False)
```

```python
import jax
import jax.numpy as jnp
from jax import lax
from jax.experimental import pallas as pl
from jax.experimental.pallas import tpu as pltpu
from jax.sharding import Mesh
from jax.sharding import PartitionSpec as P


PB = 512
LANES = 128
SUBLANES = 8
GROUPS = LANES // SUBLANES
TILE = (SUBLANES, LANES)
BLOCKS = PB // LANES
PAIRS = BLOCKS * (BLOCKS + 1) // 2
DEPTH = ("depth_0", "depth_1")
ROW_DEPTH = ("row", "depth_0", "depth_1")
Z, Y = DEPTH
Y_SIZE = 4
WIDE = PB // LANES
SLOTS = 3
SUM_PIECE, SUM_SLOT = divmod(PAIRS * GROUPS // 2, SLOTS)
HALVES = (((0, 0), (3, 0), (3, 1), (3, 2), (3, 3)), ((1, 0), (1, 1), (2, 0), (2, 1), (2, 2)))
F32 = jnp.float32


def times_transposed(left, right):
    return lax.dot_general(
        left,
        right,
        (((1,), (1,)), ((), ())),
        precision=lax.Precision.HIGHEST,
        preferred_element_type=F32,
    )


def pair(i, j):
    return i * (i + 1) // 2 + j


def inverse_factor(load, store):
    lane = lax.broadcasted_iota(jnp.int32, (SUBLANES, LANES), 1)
    sub = lax.broadcasted_iota(jnp.int32, (SUBLANES, LANES), 0)
    whole = (SUBLANES, LANES)
    rows = [load(h) for h in range(GROUPS)]
    for g in range(GROUPS):
        first = SUBLANES * g
        cols = {
            h: [
                jnp.broadcast_to(rows[h][:, first + j : first + j + 1], whole)
                for j in range(SUBLANES)
            ]
            for h in range(g, GROUPS)
        }
        inside = (lane >= first) & (lane < first + SUBLANES)
        rows[g] = jnp.where(inside, jnp.where(lane - first == sub, 1.0, 0.0), rows[g])
        for h in range(g + 1, GROUPS):
            rows[h] = jnp.where(inside, 0.0, rows[h])
        done = jnp.zeros(whole, F32)
        for j in range(SUBLANES):
            scale = lax.rsqrt(jnp.broadcast_to(cols[g][j][j : j + 1], whole))
            row = jnp.broadcast_to(rows[g][j : j + 1], whole) * scale
            done = jnp.where(sub == j, row, done)
            own = cols[g][j] * scale
            spread = {
                k: jnp.broadcast_to(own[k : k + 1], whole) for k in range(j + 1, SUBLANES)
            }
            for k in spread:
                cols[g][k] = cols[g][k] - own * spread[k]
            rows[g] = rows[g] - jnp.where(sub > j, own, 0.0) * row
            for h in range(g + 1, GROUPS):
                below = cols[h][j] * scale
                rows[h] = rows[h] - below * row
                for k in spread:
                    cols[h][k] = cols[h][k] - below * spread[k]
        store(g, jnp.where(lane <= first + sub, done, 0.0))


def halves(value):
    high = value.astype(jnp.bfloat16)
    return high, (value - high.astype(F32)).astype(jnp.bfloat16)


def product(left, right):
    def dot(a, b):
        return lax.dot_general(a, b, (((1,), (1,)), ((), ())), preferred_element_type=F32)

    return dot(left[0], right[0]) + (dot(left[0], right[1]) + dot(left[1], right[0]))


def top_kernel(place_ref, near_ref, top_in_ref, out_ref, own_ref, top_ref, all_ref, sem):
    r, c = place_ref[0], place_ref[1]
    count = own_ref.shape[0]
    first = pl.multiple_of(c * count, count)
    own = pltpu.make_async_copy(near_ref.at[pl.ds(first, count)], own_ref, sem.at[0])
    every = pltpu.make_async_copy(near_ref, all_ref, sem.at[2])
    own.start()

    @pl.when(r == 0)
    def _():
        pltpu.make_async_copy(near_ref.at[pl.ds(0, PB)], top_ref, sem.at[1]).start()

    @pl.when(r != 0)
    def _():
        pltpu.make_async_copy(top_in_ref, top_ref, sem.at[1]).start()

    every.start()
    own.wait()
    pltpu.make_async_copy(top_in_ref, top_ref, sem.at[1]).wait()
    right = halves(top_ref[...])
    value = product(halves(own_ref[...]), right)
    for d in range(32):
        for l in range(WIDE):
            out_ref[d, SLOTS + l] = value[
                SUBLANES * d : SUBLANES * (d + 1), LANES * l : LANES * (l + 1)
            ]
    for half in range(2):

        @pl.when(r == half)
        def _(half=half):
            levels = sorted({i for i, _ in HALVES[half]})
            left = tuple(
                jnp.concatenate([x[LANES * i : LANES * (i + 1)] for i in levels]) for x in right
            )
            value = product(left, right)
            for b, (i, j) in enumerate(HALVES[half]):
                for h in range(GROUPS):
                    d, k = divmod(b * GROUPS + h, SLOTS)
                    row = LANES * levels.index(i) + SUBLANES * h
                    out_ref[d, k] = value[row : row + SUBLANES, LANES * j : LANES * (j + 1)]

    for t in range(PAIRS * GROUPS // 2 + 1, 32 * SLOTS):
        out_ref[t // SLOTS, t % SLOTS] = jnp.zeros(TILE, F32)
    every.wait()
    folded = jnp.zeros((all_ref.shape[0], LANES), F32)
    for l in range(all_ref.shape[1] // LANES):
        part = all_ref[:, LANES * l : LANES * (l + 1)]
        folded = folded + part * part
    ones = jnp.ones((SUBLANES, LANES), jnp.bfloat16)
    high, low = halves(folded)

    def row_sums(part):
        return lax.dot_general(ones, part, (((1,), (1,)), ((), ())), preferred_element_type=F32)

    sums = row_sums(high) + row_sums(low)
    sub = lax.broadcasted_iota(jnp.int32, TILE, 0)
    tile = jnp.zeros(TILE, F32)
    for a in range(SUBLANES):
        tile = jnp.where(sub == a, sums[:, LANES * a : LANES * (a + 1)], tile)
    out_ref[SUM_PIECE, SUM_SLOT] = tile


def a_kernel(place_ref, a_ref, *refs):
    cols = 4
    outs = refs[:cols]
    tile_buf, panel_buf, own_buf, sem = refs[cols:]
    r, c, d = place_ref[0], place_ref[1], place_ref[2] * Y_SIZE + place_ref[3]
    copies = []
    for k in range(SLOTS):
        t = jnp.minimum(d * SLOTS + k, PAIRS * GROUPS // 2 - 1)
        b, h = t // GROUPS, lax.rem(t, GROUPS)
        places = (
            (jnp.where(b == 0, 0, 3), jnp.where(b == 0, 0, b - 1)),
            (jnp.where(b < 2, 1, 2), jnp.where(b < 2, b, b - 2)),
        )
        for half, (i, j) in enumerate(places):
            row = pl.multiple_of(i * LANES + h * SUBLANES, SUBLANES)
            col = pl.multiple_of(j * LANES, LANES)
            copies.append(
                (a_ref.at[pl.ds(row, SUBLANES), pl.ds(col, LANES)], tile_buf.at[half * SLOTS + k])
            )
    for s in range(cols):
        row = pl.multiple_of(lax.rem(c + s, cols) * 256 + d * SUBLANES, SUBLANES)
        copies.append((a_ref.at[pl.ds(row, SUBLANES), :], panel_buf.at[s]))
    for b in range(BLOCKS):
        row = pl.multiple_of(lax.rem(c, 2) * PB + b * LANES, LANES)
        copies.append((a_ref.at[pl.ds(row, LANES), pl.ds(b * LANES, LANES)], own_buf.at[b]))
    copies = [pltpu.make_async_copy(a, b, sem.at[n]) for n, (a, b) in enumerate(copies)]
    for copy in copies:
        copy.start()
    for copy in copies:
        copy.wait()
    lane = lax.broadcasted_iota(jnp.int32, (LANES, LANES), 1)
    sub = lax.broadcasted_iota(jnp.int32, (LANES, LANES), 0)
    level = lax.broadcasted_iota(jnp.int32, TILE, 0)
    diagonal = jnp.zeros(TILE, F32)
    for b in range(BLOCKS):
        values = jnp.sum(jnp.where(lane == sub, own_buf[b], 0.0), axis=0, keepdims=True)
        here = (level == lax.rem(c, 2) * BLOCKS + b) & (c // 2 == r)
        diagonal = jnp.where(here, jnp.broadcast_to(values, TILE), diagonal)
    root = c == 0
    for s in range(cols):
        for k in range(2 * SLOTS):
            outs[s][k] = jnp.where(root, tile_buf[k], 0.0)
        for l in range(WIDE):
            outs[s][2 * SLOTS + l] = jnp.where(
                root, panel_buf[s, :, LANES * l : LANES * (l + 1)], 0.0
            )
        outs[s][2 * SLOTS + WIDE] = diagonal


def merge_kernel(place_ref, got_ref, a_ref, other_ref, out_ref):
    r, d = place_ref[0], place_ref[2] * Y_SIZE + place_ref[3]
    total = got_ref[0]
    for n in range(1, got_ref.shape[0]):
        total = total + got_ref[n]
    tiles = []
    for k in range(SLOTS):
        a = jnp.where(r == 0, a_ref[k], other_ref[k])
        if k == SUM_SLOT:
            special = d == SUM_PIECE
            value = jnp.where(special, a_ref[2 * SLOTS + WIDE], a) - total[k]
            squares = jnp.sum(jnp.sum(value * value, axis=1, keepdims=True), axis=0, keepdims=True)
            tiles.append(jnp.where(special, jnp.broadcast_to(squares, TILE), value))
        else:
            tiles.append(a - total[k])
    for l in range(WIDE):
        tiles.append(a_ref[2 * SLOTS + l] - total[SLOTS + l])
    for n in range(out_ref.shape[0]):
        for k, tile in enumerate(tiles):
            out_ref[n, k] = tile


def block_kernel(place_ref, left_ref, near_ref, far_ref, *refs):
    outs, high_ref, low_ref, right_ref, sem = refs[:Y_SIZE], *refs[Y_SIZE:]
    r, c, y = place_ref[0], place_ref[1], place_ref[3]
    step = pl.program_id(0)
    here = c // 2 == r
    half = pl.multiple_of(lax.rem(c, 2) * PB, PB)

    @pl.when(step == 0)
    def _():
        @pl.when(here)
        def _():
            pltpu.make_async_copy(near_ref.at[pl.ds(half, PB)], right_ref, sem).start()

        @pl.when(jnp.logical_not(here))
        def _():
            pltpu.make_async_copy(far_ref.at[pl.ds(half, PB)], right_ref, sem).start()

        pltpu.make_async_copy(near_ref.at[pl.ds(half, PB)], right_ref, sem).wait()
        high, low = halves(right_ref[...])
        high_ref[...] = high
        low_ref[...] = low

    value = product(halves(left_ref[...]), (high_ref[...], low_ref[...]))
    for yy in range(Y_SIZE):
        for s in range(Y_SIZE):

            @pl.when(lax.rem(yy - y + Y_SIZE, Y_SIZE) == s)
            def _(yy=yy, s=s):
                for zz in range(outs[s].shape[0]):
                    for g in range(4):
                        for l in range(WIDE):
                            row = LANES * zz + 32 * yy + SUBLANES * g
                            outs[s][zz, g * WIDE + l] = value[
                                row : row + SUBLANES, LANES * l : LANES * (l + 1)
                            ]


def at(i, j):
    return slice(LANES * pair(i, j), LANES * (pair(i, j) + 1))


def block(i):
    return slice(LANES * i, LANES * (i + 1))


def solve_kernel(place_ref, mine_ref, other_ref, x_ref, norm_ref, w):
    r = place_ref[0]
    for half in range(2):
        for ref, take in ((mine_ref, r == half), (other_ref, r != half)):

            @pl.when(take)
            def _(half=half, ref=ref):
                for b, (i, j) in enumerate(HALVES[half]):
                    for h in range(GROUPS):
                        d, k = divmod(b * GROUPS + h, SLOTS)
                        row = LANES * pair(i, j) + SUBLANES * h
                        w[row : row + SUBLANES] = ref[d, k]

    for d in range(mine_ref.shape[0]):
        for l in range(WIDE):
            x_ref[SUBLANES * d : SUBLANES * (d + 1), block(l)] = mine_ref[d, SLOTS + l]
    total = mine_ref[SUM_PIECE, SUM_SLOT] + other_ref[SUM_PIECE, SUM_SLOT]
    norm_ref[0] = jnp.sqrt(total / 2048.0)[0, 0]

    low = {(i, j): w[at(i, j)] for i in range(BLOCKS) for j in range(i + 1)}
    rows = [x_ref[:, block(l)] for l in range(WIDE)]
    for s in range(BLOCKS):
        parts = [None] * GROUPS

        def load(h, square=low[s, s]):
            return square[SUBLANES * h : SUBLANES * (h + 1)]

        inverse_factor(load, parts.__setitem__)
        inv = jnp.concatenate(parts)
        for i in range(s + 1, BLOCKS):
            low[i, s] = times_transposed(low[i, s], inv)
        for j in range(s + 1, BLOCKS):
            for i in range(j, BLOCKS):
                low[i, j] = low[i, j] - times_transposed(low[i, s], low[j, s])
        x = times_transposed(rows[s], inv)
        x_ref[:, block(s)] = x
        for j in range(s + 1, BLOCKS):
            rows[j] = rows[j] - times_transposed(x, low[j, s])


SMEM = pl.BlockSpec(memory_space=pltpu.SMEM)
VMEM = pl.BlockSpec(memory_space=pltpu.VMEM)
ANY = pl.BlockSpec(memory_space=pl.ANY)


def shaped(*dims):
    return jax.ShapeDtypeStruct(dims, F32)


def call(kernel, flops, outs, in_specs, scratch=(), grid=(), out_spec=None, out_specs=None):
    out_specs = out_specs or [out_spec or VMEM] * len(outs)
    return pl.pallas_call(
        kernel,
        out_shape=outs,
        grid=grid,
        in_specs=in_specs,
        out_specs=out_specs,
        scratch_shapes=scratch,
        cost_estimate=pl.CostEstimate(flops=flops, bytes_accessed=4_000_000, transcendentals=0),
    )


def exchange(pieces, axis):
    return lax.all_to_all(pieces, axis, split_axis=0, concat_axis=0, tiled=True)


def shifted(value, axis, by):
    size = lax.axis_size(axis)
    return lax.ppermute(value, axis, [(i, (i + by) % size) for i in range(size)])


def delivered(pieces, axis):
    return [pieces[0]] + [shifted(pieces[s], axis, s) for s in range(1, len(pieces))]


def body(a_tile, panels):
    tile_rows, tile_cols = a_tile.shape
    z_size, depth = lax.axis_size(Z), lax.axis_size(DEPTH)
    c_rows = tile_rows // 4
    share = tile_rows // depth
    k_size = panels.shape[1]
    r, c = lax.axis_index("row"), lax.axis_index("col")
    place = jnp.stack([r, c, lax.axis_index(Z), lax.axis_index(Y)]).astype(jnp.int32)
    swap = [(0, 1), (1, 0)]

    top = lax.ppermute(panels[:PB], "row", [(0, 1)])
    far = lax.ppermute(panels, "row", swap)

    piece = shaped(depth, SLOTS + WIDE, *TILE)
    (part,) = call(
        top_kernel,
        8_000_000_000,
        [piece],
        [SMEM, ANY, ANY],
        [
            pltpu.VMEM((c_rows, k_size), F32),
            pltpu.VMEM((PB, k_size), F32),
            pltpu.VMEM((tile_rows, k_size), F32),
            pltpu.SemaphoreType.DMA((3,)),
        ],
    )(place, panels, top)
    got = exchange(part, DEPTH)

    a_sent = call(
        a_kernel,
        1_000_000_000,
        [shaped(2 * SLOTS + WIDE + 1, *TILE)] * 4,
        [SMEM, ANY],
        [
            pltpu.VMEM((2 * SLOTS, *TILE), F32),
            pltpu.VMEM((4, SUBLANES, PB), F32),
            pltpu.VMEM((BLOCKS, LANES, LANES), F32),
            pltpu.SemaphoreType.DMA((2 * SLOTS + 4 + BLOCKS,)),
        ],
    )(place, a_tile)
    a_got = delivered(a_sent, "col")
    a_got = sum(a_got)
    a_other = lax.ppermute(a_got[SLOTS : 2 * SLOTS], "row", [(0, 1)])

    (piece_copies,) = call(
        merge_kernel, 1_000_000_000, [piece], [SMEM, VMEM, VMEM, VMEM]
    )(place, got, a_got, a_other)
    mine = exchange(piece_copies, DEPTH)
    other = lax.ppermute(mine[:, :SLOTS], "row", swap)

    piece = shaped(z_size, 4 * WIDE, *TILE)
    parts = call(
        block_kernel,
        20_000_000_000,
        [piece] * Y_SIZE,
        [SMEM, pl.BlockSpec((PB, k_size), lambda i: (i, 0)), ANY, ANY],
        [
            pltpu.VMEM((PB, k_size), jnp.bfloat16),
            pltpu.VMEM((PB, k_size), jnp.bfloat16),
            pltpu.VMEM((PB, k_size), F32),
            pltpu.SemaphoreType.DMA,
        ],
        grid=(2,),
        out_spec=pl.BlockSpec((z_size // 2, *piece.shape[1:]), lambda i: (i, 0, 0, 0)),
    )(place, panels, panels, far)
    parts = delivered(parts, Y)
    part = sum(parts)
    got = exchange(part, Z)
    tiles = got.sum(axis=0)
    tiles = tiles.reshape(4, WIDE, *TILE).transpose(0, 2, 1, 3).reshape(share, tile_cols)
    d = lax.axis_index(DEPTH)
    trailing = lax.dynamic_slice_in_dim(a_tile, d * share, share, 0) - tiles

    new_panel, norm = call(
        solve_kernel,
        30_000_000_000,
        [shaped(c_rows, PB), shaped(1)],
        [SMEM, VMEM, VMEM],
        [pltpu.VMEM((PAIRS * LANES, LANES), F32)],
        out_specs=[VMEM, SMEM],
    )(place, mine, other)
    return (trailing, new_panel, norm)


def solution(mesh):
    finer = Mesh(
        mesh.devices.reshape(mesh.shape["row"], mesh.shape["col"], 8, 4),
        ("row", "col", "depth_0", "depth_1"),
    )
    in_specs = (P("row", "col"), P("row", DEPTH))
    out_specs = (P(ROW_DEPTH, "col"), P(("row", "col"), None), P())
    return jax.shard_map(body, mesh=finer, in_specs=in_specs, out_specs=out_specs, check_vma=False)
```

```python
import jax
import jax.numpy as jnp
from jax import lax
from jax.experimental import pallas as pl
from jax.experimental.pallas import tpu as pltpu
from jax.sharding import Mesh
from jax.sharding import PartitionSpec as P


PB = 512
LANES = 128
SUBLANES = 8
GROUPS = LANES // SUBLANES
TILE = (SUBLANES, LANES)
BLOCKS = PB // LANES
PAIRS = BLOCKS * (BLOCKS + 1) // 2
DEPTH = ("depth_0", "depth_1")
ROW_DEPTH = ("row", "depth_0", "depth_1")
Z, Y = DEPTH
Y_SIZE = 4
WIDE = PB // LANES
SLOTS = 3
SUM_PIECE, SUM_SLOT = divmod(PAIRS * GROUPS // 2, SLOTS)
HALVES = (((0, 0), (3, 0), (3, 1), (3, 2), (3, 3)), ((1, 0), (1, 1), (2, 0), (2, 1), (2, 2)))
F32 = jnp.float32


def times_transposed(left, right):
    return lax.dot_general(
        left,
        right,
        (((1,), (1,)), ((), ())),
        precision=lax.Precision.HIGHEST,
        preferred_element_type=F32,
    )


def pair(i, j):
    return i * (i + 1) // 2 + j


def inverse_factor(load, store):
    lane = lax.broadcasted_iota(jnp.int32, TILE, 1)
    sub = lax.broadcasted_iota(jnp.int32, TILE, 0)

    def spread_columns(row, g):
        first = SUBLANES * g
        return [
            jnp.broadcast_to(row[:, first + j : first + j + 1], TILE) for j in range(SUBLANES)
        ]

    rows = [load(h) for h in range(GROUPS)]
    cols = {(h, 0): spread_columns(rows[h], 0) for h in range(GROUPS)}
    for h in (1, 2):
        cols[h, 1] = spread_columns(rows[h], 1)
    for g in range(GROUPS):
        first = SUBLANES * g
        inside = (lane >= first) & (lane < first + SUBLANES)
        own = cols.pop((g, g))
        row = jnp.where(inside, jnp.where(lane - first == sub, 1.0, 0.0), rows[g])
        done = jnp.zeros(TILE, F32)
        scales, spreads, finals = [], [], []
        for j in range(SUBLANES):
            scale = lax.rsqrt(jnp.broadcast_to(own[j][j : j + 1], TILE))
            final = jnp.broadcast_to(row[j : j + 1], TILE) * scale
            done = jnp.where(sub == j, final, done)
            factor = own[j] * scale
            spread = {k: jnp.broadcast_to(factor[k : k + 1], TILE) for k in range(j + 1, SUBLANES)}
            for k in spread:
                own[k] = own[k] - factor * spread[k]
            row = row - jnp.where(sub > j, factor, 0.0) * final
            scales.append(scale)
            spreads.append(spread)
            finals.append(final)
        store(g, jnp.where(lane <= first + sub, done, 0.0))
        ahead = []
        for h in range(g + 1, GROUPS):
            row = jnp.where(inside, 0.0, rows[h])
            here = cols.pop((h, g))
            factors = []
            for j in range(SUBLANES):
                factor = here[j] * scales[j]
                for k in spreads[j]:
                    here[k] = here[k] - factor * spreads[j][k]
                row = row - factor * finals[j]
                factors.append(factor)
            rows[h] = row
            if h == g + 1:
                ahead = [
                    [jnp.broadcast_to(f[k : k + 1], TILE) for k in range(SUBLANES)] for f in factors
                ]
            if h <= g + 2:
                late = cols[h, g + 1]
                for j in range(SUBLANES):
                    for k in range(SUBLANES):
                        late[k] = late[k] - factors[j] * ahead[j][k]
            else:
                cols[h, g + 1] = spread_columns(row, g + 1)
            if g + 2 <= h <= g + 3:
                cols[h, g + 2] = spread_columns(row, g + 2)


def halves(value):
    high = value.astype(jnp.bfloat16)
    return high, (value - high.astype(F32)).astype(jnp.bfloat16)


def product(left, right):
    def dot(a, b):
        return lax.dot_general(a, b, (((1,), (1,)), ((), ())), preferred_element_type=F32)

    return dot(left[0], right[0]) + (dot(left[0], right[1]) + dot(left[1], right[0]))


def top_kernel(place_ref, near_ref, top_in_ref, hbm_ref, own_ref, top_ref, all_ref, out_ref, sem):
    r, c = place_ref[0], place_ref[1]
    count = own_ref.shape[0]
    first = pl.multiple_of(c * count, count)
    own = pltpu.make_async_copy(near_ref.at[pl.ds(first, count)], own_ref, sem.at[0])
    every = pltpu.make_async_copy(near_ref, all_ref, sem.at[2])
    own.start()

    @pl.when(r == 0)
    def _():
        pltpu.make_async_copy(near_ref.at[pl.ds(0, PB)], top_ref, sem.at[1]).start()

    @pl.when(r != 0)
    def _():
        pltpu.make_async_copy(top_in_ref, top_ref, sem.at[1]).start()

    every.start()
    own.wait()
    pltpu.make_async_copy(top_in_ref, top_ref, sem.at[1]).wait()
    right = halves(top_ref[...])
    value = product(halves(own_ref[...]), right)
    for d in range(32):
        for l in range(WIDE):
            out_ref[d, SLOTS + l] = value[
                SUBLANES * d : SUBLANES * (d + 1), LANES * l : LANES * (l + 1)
            ]
    panel = pl.ds(SLOTS, WIDE)
    panel = pltpu.make_async_copy(out_ref.at[:, panel], hbm_ref.at[:, panel], sem.at[3])
    panel.start()
    for half in range(2):

        @pl.when(r == half)
        def _(half=half):
            levels = sorted({i for i, _ in HALVES[half]})
            left = tuple(
                jnp.concatenate([x[LANES * i : LANES * (i + 1)] for i in levels]) for x in right
            )
            value = product(left, right)
            for b, (i, j) in enumerate(HALVES[half]):
                for h in range(GROUPS):
                    d, k = divmod(b * GROUPS + h, SLOTS)
                    row = LANES * levels.index(i) + SUBLANES * h
                    out_ref[d, k] = value[row : row + SUBLANES, LANES * j : LANES * (j + 1)]

    for t in range(PAIRS * GROUPS // 2 + 1, 32 * SLOTS):
        out_ref[t // SLOTS, t % SLOTS] = jnp.zeros(TILE, F32)
    every.wait()
    folded = jnp.zeros((all_ref.shape[0], LANES), F32)
    for l in range(all_ref.shape[1] // LANES):
        part = all_ref[:, LANES * l : LANES * (l + 1)]
        folded = folded + part * part
    ones = jnp.ones((SUBLANES, LANES), jnp.bfloat16)
    high, low = halves(folded)

    def row_sums(part):
        return lax.dot_general(ones, part, (((1,), (1,)), ((), ())), preferred_element_type=F32)

    sums = row_sums(high) + row_sums(low)
    sub = lax.broadcasted_iota(jnp.int32, TILE, 0)
    tile = jnp.zeros(TILE, F32)
    for a in range(SUBLANES):
        tile = jnp.where(sub == a, sums[:, LANES * a : LANES * (a + 1)], tile)
    out_ref[SUM_PIECE, SUM_SLOT] = tile
    square = pl.ds(0, SLOTS)
    square = pltpu.make_async_copy(out_ref.at[:, square], hbm_ref.at[:, square], sem.at[4])
    square.start()
    panel.wait()
    square.wait()


def a_kernel(place_ref, a_ref, *refs):
    cols = 4
    outs = refs[:cols]
    tile_buf, panel_buf, own_buf, sem = refs[cols:]
    r, c, d = place_ref[0], place_ref[1], place_ref[2] * Y_SIZE + place_ref[3]
    copies = []
    for k in range(SLOTS):
        t = jnp.minimum(d * SLOTS + k, PAIRS * GROUPS // 2 - 1)
        b, h = t // GROUPS, lax.rem(t, GROUPS)
        places = (
            (jnp.where(b == 0, 0, 3), jnp.where(b == 0, 0, b - 1)),
            (jnp.where(b < 2, 1, 2), jnp.where(b < 2, b, b - 2)),
        )
        for half, (i, j) in enumerate(places):
            row = pl.multiple_of(i * LANES + h * SUBLANES, SUBLANES)
            col = pl.multiple_of(j * LANES, LANES)
            copies.append(
                (a_ref.at[pl.ds(row, SUBLANES), pl.ds(col, LANES)], tile_buf.at[half * SLOTS + k])
            )
    for s in range(cols):
        row = pl.multiple_of(lax.rem(c + s, cols) * 256 + d * SUBLANES, SUBLANES)
        copies.append((a_ref.at[pl.ds(row, SUBLANES), :], panel_buf.at[s]))
    for b in range(BLOCKS):
        row = pl.multiple_of(lax.rem(c, 2) * PB + b * LANES, LANES)
        copies.append((a_ref.at[pl.ds(row, LANES), pl.ds(b * LANES, LANES)], own_buf.at[b]))
    copies = [pltpu.make_async_copy(a, b, sem.at[n]) for n, (a, b) in enumerate(copies)]
    for copy in copies:
        copy.start()
    for copy in copies:
        copy.wait()
    lane = lax.broadcasted_iota(jnp.int32, (LANES, LANES), 1)
    sub = lax.broadcasted_iota(jnp.int32, (LANES, LANES), 0)
    level = lax.broadcasted_iota(jnp.int32, TILE, 0)
    diagonal = jnp.zeros(TILE, F32)
    for b in range(BLOCKS):
        values = jnp.sum(jnp.where(lane == sub, own_buf[b], 0.0), axis=0, keepdims=True)
        here = (level == lax.rem(c, 2) * BLOCKS + b) & (c // 2 == r)
        diagonal = jnp.where(here, jnp.broadcast_to(values, TILE), diagonal)
    root = c == 0
    for s in range(cols):
        for k in range(2 * SLOTS):
            outs[s][k] = jnp.where(root, tile_buf[k], 0.0)
        for l in range(WIDE):
            outs[s][2 * SLOTS + l] = jnp.where(
                root, panel_buf[s, :, LANES * l : LANES * (l + 1)], 0.0
            )
        outs[s][2 * SLOTS + WIDE] = diagonal


def merge_kernel(place_ref, got_ref, a_ref, other_ref, out_ref, got_buf, a_buf, other_buf, piece, sem):
    r, d = place_ref[0], place_ref[2] * Y_SIZE + place_ref[3]
    count = got_ref.shape[0]
    chunk = count // 4
    loads = [
        pltpu.make_async_copy(
            got_ref.at[pl.ds(chunk * n, chunk)], got_buf.at[pl.ds(chunk * n, chunk)], sem.at[n]
        )
        for n in range(4)
    ]
    loads.append(pltpu.make_async_copy(a_ref, a_buf, sem.at[4]))
    loads.append(pltpu.make_async_copy(other_ref, other_buf, sem.at[5]))
    for load in loads:
        load.start()
    total = [jnp.zeros(TILE, F32)] * (SLOTS + WIDE)
    for n in range(4):
        loads[n].wait()
        for m in range(chunk * n, chunk * (n + 1)):
            total = [t + got_buf[m, k] for k, t in enumerate(total)]
    loads[4].wait()
    loads[5].wait()
    for k in range(SLOTS):
        a = jnp.where(r == 0, a_buf[k], other_buf[k])
        if k == SUM_SLOT:
            special = d == SUM_PIECE
            value = jnp.where(special, a_buf[2 * SLOTS + WIDE], a) - total[k]
            squares = jnp.sum(jnp.sum(value * value, axis=1, keepdims=True), axis=0, keepdims=True)
            piece[k] = jnp.where(special, jnp.broadcast_to(squares, TILE), value)
        else:
            piece[k] = a - total[k]
    for l in range(WIDE):
        piece[SLOTS + l] = a_buf[2 * SLOTS + l] - total[SLOTS + l]
    stores = [
        pltpu.make_async_copy(piece, out_ref.at[n], sem.at[6 + n]) for n in range(out_ref.shape[0])
    ]
    for store in stores:
        store.start()
    for store in stores:
        store.wait()


def block_kernel(place_ref, left_ref, near_ref, far_ref, *refs):
    outs, high_ref, low_ref, right_ref, sem = refs[:Y_SIZE], *refs[Y_SIZE:]
    r, c, y = place_ref[0], place_ref[1], place_ref[3]
    step = pl.program_id(0)
    here = c // 2 == r
    half = pl.multiple_of(lax.rem(c, 2) * PB, PB)

    @pl.when(step == 0)
    def _():
        @pl.when(here)
        def _():
            pltpu.make_async_copy(near_ref.at[pl.ds(half, PB)], right_ref, sem).start()

        @pl.when(jnp.logical_not(here))
        def _():
            pltpu.make_async_copy(far_ref.at[pl.ds(half, PB)], right_ref, sem).start()

        pltpu.make_async_copy(near_ref.at[pl.ds(half, PB)], right_ref, sem).wait()
        high, low = halves(right_ref[...])
        high_ref[...] = high
        low_ref[...] = low

    value = product(halves(left_ref[...]), (high_ref[...], low_ref[...]))
    for yy in range(Y_SIZE):
        for s in range(Y_SIZE):

            @pl.when(lax.rem(yy - y + Y_SIZE, Y_SIZE) == s)
            def _(yy=yy, s=s):
                for zz in range(outs[s].shape[0]):
                    for g in range(4):
                        for l in range(WIDE):
                            row = LANES * zz + 32 * yy + SUBLANES * g
                            outs[s][zz, g * WIDE + l] = value[
                                row : row + SUBLANES, LANES * l : LANES * (l + 1)
                            ]


def at(i, j):
    return slice(LANES * pair(i, j), LANES * (pair(i, j) + 1))


def block(i):
    return slice(LANES * i, LANES * (i + 1))


def solve_kernel(place_ref, mine_in_ref, other_in_ref, x_ref, norm_ref, other_ref, mine_ref, w, sem):
    r = place_ref[0]
    load = pltpu.make_async_copy(other_in_ref.at[:, pl.ds(0, SLOTS)], other_ref, sem.at[0])
    load.start()
    own = pltpu.make_async_copy(mine_in_ref, mine_ref, sem.at[1])
    own.start()
    own.wait()
    for d in range(mine_ref.shape[0]):
        for l in range(WIDE):
            x_ref[SUBLANES * d : SUBLANES * (d + 1), block(l)] = mine_ref[d, SLOTS + l]
    load.wait()
    for half in range(2):
        for ref, take in ((mine_ref, r == half), (other_ref, r != half)):

            @pl.when(take)
            def _(half=half, ref=ref):
                for b, (i, j) in enumerate(HALVES[half]):
                    for h in range(GROUPS):
                        d, k = divmod(b * GROUPS + h, SLOTS)
                        row = LANES * pair(i, j) + SUBLANES * h
                        w[row : row + SUBLANES] = ref[d, k]

    total = mine_ref[SUM_PIECE, SUM_SLOT] + other_ref[SUM_PIECE, SUM_SLOT]
    norm_ref[0] = jnp.sqrt(total / 2048.0)[0, 0]

    low = {(i, j): w[at(i, j)] for i in range(BLOCKS) for j in range(i + 1)}
    rows = [x_ref[:, block(l)] for l in range(WIDE)]
    for s in range(BLOCKS):
        parts = [None] * GROUPS

        def load(h, square=low[s, s]):
            return square[SUBLANES * h : SUBLANES * (h + 1)]

        inverse_factor(load, parts.__setitem__)
        inv = jnp.concatenate(parts)
        for i in range(s + 1, BLOCKS):
            low[i, s] = times_transposed(low[i, s], inv)
        for j in range(s + 1, BLOCKS):
            for i in range(j, BLOCKS):
                low[i, j] = low[i, j] - times_transposed(low[i, s], low[j, s])
        x = times_transposed(rows[s], inv)
        x_ref[:, block(s)] = x
        for j in range(s + 1, BLOCKS):
            rows[j] = rows[j] - times_transposed(x, low[j, s])


SMEM = pl.BlockSpec(memory_space=pltpu.SMEM)
VMEM = pl.BlockSpec(memory_space=pltpu.VMEM)
ANY = pl.BlockSpec(memory_space=pl.ANY)


def shaped(*dims):
    return jax.ShapeDtypeStruct(dims, F32)


def call(kernel, flops, outs, in_specs, scratch=(), grid=(), out_spec=None, out_specs=None, room=None):
    out_specs = out_specs or [out_spec or VMEM] * len(outs)
    return pl.pallas_call(
        kernel,
        out_shape=outs,
        grid=grid,
        in_specs=in_specs,
        out_specs=out_specs,
        scratch_shapes=scratch,
        compiler_params=pltpu.CompilerParams(vmem_limit_bytes=room),
        cost_estimate=pl.CostEstimate(flops=flops, bytes_accessed=4_000_000, transcendentals=0),
    )


def exchange(pieces, axis):
    return lax.all_to_all(pieces, axis, split_axis=0, concat_axis=0, tiled=True)


def shifted(value, axis, by):
    size = lax.axis_size(axis)
    return lax.ppermute(value, axis, [(i, (i + by) % size) for i in range(size)])


def delivered(pieces, axis):
    return [pieces[0]] + [shifted(pieces[s], axis, s) for s in range(1, len(pieces))]


def body(a_tile, panels):
    tile_rows, tile_cols = a_tile.shape
    z_size, depth = lax.axis_size(Z), lax.axis_size(DEPTH)
    c_rows = tile_rows // 4
    share = tile_rows // depth
    k_size = panels.shape[1]
    r, c = lax.axis_index("row"), lax.axis_index("col")
    place = jnp.stack([r, c, lax.axis_index(Z), lax.axis_index(Y)]).astype(jnp.int32)
    swap = [(0, 1), (1, 0)]

    top = lax.ppermute(panels[:PB], "row", [(0, 1)])
    far = lax.ppermute(panels, "row", swap)

    piece = shaped(depth, SLOTS + WIDE, *TILE)
    (part,) = call(
        top_kernel,
        8_000_000_000,
        [piece],
        [SMEM, ANY, ANY],
        [
            pltpu.VMEM((c_rows, k_size), F32),
            pltpu.VMEM((PB, k_size), F32),
            pltpu.VMEM((tile_rows, k_size), F32),
            pltpu.VMEM(piece.shape, F32),
            pltpu.SemaphoreType.DMA((5,)),
        ],
        out_specs=[ANY],
        room=32 << 20,
    )(place, panels, top)
    got = exchange(part, DEPTH)

    a_sent = call(
        a_kernel,
        1_000_000_000,
        [shaped(2 * SLOTS + WIDE + 1, *TILE)] * 4,
        [SMEM, ANY],
        [
            pltpu.VMEM((2 * SLOTS, *TILE), F32),
            pltpu.VMEM((4, SUBLANES, PB), F32),
            pltpu.VMEM((BLOCKS, LANES, LANES), F32),
            pltpu.SemaphoreType.DMA((2 * SLOTS + 4 + BLOCKS,)),
        ],
    )(place, a_tile)
    a_got = delivered(a_sent, "col")
    a_got = sum(a_got)
    a_other = lax.ppermute(a_got[SLOTS : 2 * SLOTS], "row", [(0, 1)])

    (piece_copies,) = call(
        merge_kernel,
        1_000_000_000,
        [piece],
        [SMEM, ANY, ANY, ANY],
        [
            pltpu.VMEM(piece.shape, F32),
            pltpu.VMEM(a_got.shape, F32),
            pltpu.VMEM(a_other.shape, F32),
            pltpu.VMEM(piece.shape[1:], F32),
            pltpu.SemaphoreType.DMA((6 + depth,)),
        ],
        out_specs=[ANY],
        room=8 << 20,
    )(place, got, a_got, a_other)
    mine = exchange(piece_copies, DEPTH)
    other = lax.ppermute(mine, "row", swap)

    piece = shaped(z_size, 4 * WIDE, *TILE)
    parts = call(
        block_kernel,
        20_000_000_000,
        [piece] * Y_SIZE,
        [SMEM, pl.BlockSpec((PB, k_size), lambda i: (i, 0)), ANY, ANY],
        [
            pltpu.VMEM((PB, k_size), jnp.bfloat16),
            pltpu.VMEM((PB, k_size), jnp.bfloat16),
            pltpu.VMEM((PB, k_size), F32),
            pltpu.SemaphoreType.DMA,
        ],
        grid=(2,),
        out_spec=pl.BlockSpec((z_size // 2, *piece.shape[1:]), lambda i: (i, 0, 0, 0)),
        room=32 << 20,
    )(place, panels, panels, far)
    parts = delivered(parts, Y)
    part = sum(parts)
    got = exchange(part, Z)
    tiles = got.sum(axis=0)
    tiles = tiles.reshape(4, WIDE, *TILE).transpose(0, 2, 1, 3).reshape(share, tile_cols)
    d = lax.axis_index(DEPTH)
    trailing = lax.dynamic_slice_in_dim(a_tile, d * share, share, 0) - tiles

    new_panel, norm = call(
        solve_kernel,
        30_000_000_000,
        [shaped(c_rows, PB), shaped(1)],
        [SMEM, ANY, ANY],
        [
            pltpu.VMEM((depth, SLOTS, *TILE), F32),
            pltpu.VMEM(mine.shape, F32),
            pltpu.VMEM((PAIRS * LANES, LANES), F32),
            pltpu.SemaphoreType.DMA((2,)),
        ],
        out_specs=[VMEM, SMEM],
        room=24 << 20,
    )(place, mine, other)
    return (trailing, new_panel, norm)


def solution(mesh):
    finer = Mesh(
        mesh.devices.reshape(mesh.shape["row"], mesh.shape["col"], 8, 4),
        ("row", "col", "depth_0", "depth_1"),
    )
    in_specs = (P("row", "col"), P("row", DEPTH))
    out_specs = (P(ROW_DEPTH, "col"), P(("row", "col"), None), P())
    return jax.shard_map(body, mesh=finer, in_specs=in_specs, out_specs=out_specs, check_vma=False)
```

```python
import jax
import jax.numpy as jnp
from jax import lax
from jax.experimental import pallas as pl
from jax.experimental.pallas import tpu as pltpu
from jax.sharding import Mesh
from jax.sharding import PartitionSpec as P


PB = 512
LANES = 128
SUBLANES = 8
GROUPS = LANES // SUBLANES
TILE = (SUBLANES, LANES)
BLOCKS = PB // LANES
PAIRS = BLOCKS * (BLOCKS + 1) // 2
DEPTH = ("depth_0", "depth_1")
ROW_DEPTH = ("row", "depth_0", "depth_1")
Z, Y = DEPTH
Y_SIZE = 4
WIDE = PB // LANES
SLOTS = 3
SUM_PIECE, SUM_SLOT = divmod(PAIRS * GROUPS // 2, SLOTS)
HALVES = (((0, 0), (3, 0), (3, 1), (3, 2), (3, 3)), ((1, 0), (1, 1), (2, 0), (2, 1), (2, 2)))
F32 = jnp.float32


def times_transposed(left, right):
    return lax.dot_general(
        left,
        right,
        (((1,), (1,)), ((), ())),
        precision=lax.Precision.HIGHEST,
        preferred_element_type=F32,
    )


def pair(i, j):
    return i * (i + 1) // 2 + j


def inverse_factor(load, store):
    lane = lax.broadcasted_iota(jnp.int32, TILE, 1)
    sub = lax.broadcasted_iota(jnp.int32, TILE, 0)

    def spread_columns(row, g):
        first = SUBLANES * g
        return [
            jnp.broadcast_to(row[:, first + j : first + j + 1], TILE) for j in range(SUBLANES)
        ]

    rows = [load(h) for h in range(GROUPS)]
    cols = {(h, 0): spread_columns(rows[h], 0) for h in range(GROUPS)}
    for h in (1, 2):
        cols[h, 1] = spread_columns(rows[h], 1)
    for g in range(GROUPS):
        first = SUBLANES * g
        inside = (lane >= first) & (lane < first + SUBLANES)
        own = cols.pop((g, g))
        row = jnp.where(inside, jnp.where(lane - first == sub, 1.0, 0.0), rows[g])
        done = jnp.zeros(TILE, F32)
        scales, spreads, finals = [], [], []
        for j in range(SUBLANES):
            scale = lax.rsqrt(jnp.broadcast_to(own[j][j : j + 1], TILE))
            final = jnp.broadcast_to(row[j : j + 1], TILE) * scale
            done = jnp.where(sub == j, final, done)
            factor = own[j] * scale
            spread = {k: jnp.broadcast_to(factor[k : k + 1], TILE) for k in range(j + 1, SUBLANES)}
            for k in spread:
                own[k] = own[k] - factor * spread[k]
            row = row - jnp.where(sub > j, factor, 0.0) * final
            scales.append(scale)
            spreads.append(spread)
            finals.append(final)
        store(g, jnp.where(lane <= first + sub, done, 0.0))
        ahead = []
        for h in range(g + 1, GROUPS):
            row = jnp.where(inside, 0.0, rows[h])
            here = cols.pop((h, g))
            factors = []
            for j in range(SUBLANES):
                factor = here[j] * scales[j]
                for k in spreads[j]:
                    here[k] = here[k] - factor * spreads[j][k]
                row = row - factor * finals[j]
                factors.append(factor)
            rows[h] = row
            if h == g + 1:
                ahead = [
                    [jnp.broadcast_to(f[k : k + 1], TILE) for k in range(SUBLANES)] for f in factors
                ]
            if h <= g + 2:
                late = cols[h, g + 1]
                for j in range(SUBLANES):
                    for k in range(SUBLANES):
                        late[k] = late[k] - factors[j] * ahead[j][k]
            else:
                cols[h, g + 1] = spread_columns(row, g + 1)
            if g + 2 <= h <= g + 3:
                cols[h, g + 2] = spread_columns(row, g + 2)


def halves(value):
    high = value.astype(jnp.bfloat16)
    return high, (value - high.astype(F32)).astype(jnp.bfloat16)


def product(left, right):
    def dot(a, b):
        return lax.dot_general(a, b, (((1,), (1,)), ((), ())), preferred_element_type=F32)

    return dot(left[0], right[0]) + (dot(left[0], right[1]) + dot(left[1], right[0]))


def top_kernel(place_ref, near_ref, far_ref, hbm_ref, own_ref, top_ref, all_ref, out_ref, sem):
    r, c = place_ref[0], place_ref[1]
    count = own_ref.shape[0]
    first = pl.multiple_of(c * count, count)
    own = pltpu.make_async_copy(near_ref.at[pl.ds(first, count)], own_ref, sem.at[0])
    every = pltpu.make_async_copy(near_ref, all_ref, sem.at[2])
    own.start()

    @pl.when(r == 0)
    def _():
        pltpu.make_async_copy(near_ref.at[pl.ds(0, PB)], top_ref, sem.at[1]).start()

    @pl.when(r != 0)
    def _():
        pltpu.make_async_copy(far_ref.at[pl.ds(0, PB)], top_ref, sem.at[1]).start()

    own.wait()
    pltpu.make_async_copy(near_ref.at[pl.ds(0, PB)], top_ref, sem.at[1]).wait()
    every.start()
    right = halves(top_ref[...])
    value = product(halves(own_ref[...]), right)
    for d in range(32):
        for l in range(WIDE):
            out_ref[d, SLOTS + l] = value[
                SUBLANES * d : SUBLANES * (d + 1), LANES * l : LANES * (l + 1)
            ]
    panel = pl.ds(SLOTS, WIDE)
    panel = pltpu.make_async_copy(out_ref.at[:, panel], hbm_ref.at[:, panel], sem.at[3])
    panel.start()
    for half in range(2):

        @pl.when(r == half)
        def _(half=half):
            levels = sorted({i for i, _ in HALVES[half]})
            left = tuple(
                jnp.concatenate([x[LANES * i : LANES * (i + 1)] for i in levels]) for x in right
            )
            value = product(left, right)
            for b, (i, j) in enumerate(HALVES[half]):
                for h in range(GROUPS):
                    d, k = divmod(b * GROUPS + h, SLOTS)
                    row = LANES * levels.index(i) + SUBLANES * h
                    out_ref[d, k] = value[row : row + SUBLANES, LANES * j : LANES * (j + 1)]

    for t in range(PAIRS * GROUPS // 2 + 1, 32 * SLOTS):
        out_ref[t // SLOTS, t % SLOTS] = jnp.zeros(TILE, F32)
    every.wait()
    folded = jnp.zeros((all_ref.shape[0], LANES), F32)
    for l in range(all_ref.shape[1] // LANES):
        part = all_ref[:, LANES * l : LANES * (l + 1)]
        folded = folded + part * part
    ones = jnp.ones((SUBLANES, LANES), jnp.bfloat16)
    high, low = halves(folded)

    def row_sums(part):
        return lax.dot_general(ones, part, (((1,), (1,)), ((), ())), preferred_element_type=F32)

    sums = row_sums(high) + row_sums(low)
    sub = lax.broadcasted_iota(jnp.int32, TILE, 0)
    tile = jnp.zeros(TILE, F32)
    for a in range(SUBLANES):
        tile = jnp.where(sub == a, sums[:, LANES * a : LANES * (a + 1)], tile)
    out_ref[SUM_PIECE, SUM_SLOT] = tile
    square = pl.ds(0, SLOTS)
    square = pltpu.make_async_copy(out_ref.at[:, square], hbm_ref.at[:, square], sem.at[4])
    square.start()
    panel.wait()
    square.wait()


def a_kernel(place_ref, a_ref, *refs):
    cols = 4
    outs = refs[:cols]
    tile_buf, panel_buf, own_buf, sem = refs[cols:]
    r, c, d = place_ref[0], place_ref[1], place_ref[2] * Y_SIZE + place_ref[3]
    copies = []
    for k in range(SLOTS):
        t = jnp.minimum(d * SLOTS + k, PAIRS * GROUPS // 2 - 1)
        b, h = t // GROUPS, lax.rem(t, GROUPS)
        places = (
            (jnp.where(b == 0, 0, 3), jnp.where(b == 0, 0, b - 1)),
            (jnp.where(b < 2, 1, 2), jnp.where(b < 2, b, b - 2)),
        )
        for half, (i, j) in enumerate(places):
            row = pl.multiple_of(i * LANES + h * SUBLANES, SUBLANES)
            col = pl.multiple_of(j * LANES, LANES)
            copies.append(
                (a_ref.at[pl.ds(row, SUBLANES), pl.ds(col, LANES)], tile_buf.at[half * SLOTS + k])
            )
    for s in range(cols):
        row = pl.multiple_of(lax.rem(c + s, cols) * 256 + d * SUBLANES, SUBLANES)
        copies.append((a_ref.at[pl.ds(row, SUBLANES), :], panel_buf.at[s]))
    for b in range(BLOCKS):
        row = pl.multiple_of(lax.rem(c, 2) * PB + b * LANES, LANES)
        copies.append((a_ref.at[pl.ds(row, LANES), pl.ds(b * LANES, LANES)], own_buf.at[b]))
    copies = [pltpu.make_async_copy(a, b, sem.at[n]) for n, (a, b) in enumerate(copies)]
    for copy in copies:
        copy.start()
    for copy in copies:
        copy.wait()
    lane = lax.broadcasted_iota(jnp.int32, (LANES, LANES), 1)
    sub = lax.broadcasted_iota(jnp.int32, (LANES, LANES), 0)
    level = lax.broadcasted_iota(jnp.int32, TILE, 0)
    diagonal = jnp.zeros(TILE, F32)
    for b in range(BLOCKS):
        values = jnp.sum(jnp.where(lane == sub, own_buf[b], 0.0), axis=0, keepdims=True)
        here = (level == lax.rem(c, 2) * BLOCKS + b) & (c // 2 == r)
        diagonal = jnp.where(here, jnp.broadcast_to(values, TILE), diagonal)
    root = c == 0
    for s in range(cols):
        for k in range(2 * SLOTS):
            outs[s][k] = jnp.where(root, tile_buf[k], 0.0)
        for l in range(WIDE):
            outs[s][2 * SLOTS + l] = jnp.where(
                root, panel_buf[s, :, LANES * l : LANES * (l + 1)], 0.0
            )
        outs[s][2 * SLOTS + WIDE] = diagonal


def merge_kernel(place_ref, got_ref, a_ref, other_ref, out_ref):
    r, d = place_ref[0], place_ref[2] * Y_SIZE + place_ref[3]
    total = [got_ref[0, k] for k in range(SLOTS + WIDE)]
    for n in range(1, got_ref.shape[0]):
        total = [t + got_ref[n, k] for k, t in enumerate(total)]
    tiles = []
    for k in range(SLOTS):
        a = jnp.where(r == 0, a_ref[k], other_ref[k])
        if k == SUM_SLOT:
            special = d == SUM_PIECE
            value = jnp.where(special, a_ref[2 * SLOTS + WIDE], a) - total[k]
            squares = jnp.sum(jnp.sum(value * value, axis=1, keepdims=True), axis=0, keepdims=True)
            tiles.append(jnp.where(special, jnp.broadcast_to(squares, TILE), value))
        else:
            tiles.append(a - total[k])
    for l in range(WIDE):
        tiles.append(a_ref[2 * SLOTS + l] - total[SLOTS + l])
    for n in range(out_ref.shape[0]):
        for k, tile in enumerate(tiles):
            out_ref[n, k] = tile


def block_kernel(place_ref, left_ref, near_ref, far_ref, *refs):
    outs, high_ref, low_ref, right_ref, sem = refs[:Y_SIZE], *refs[Y_SIZE:]
    r, c, y = place_ref[0], place_ref[1], place_ref[3]
    step = pl.program_id(0)
    here = c // 2 == r
    half = pl.multiple_of(lax.rem(c, 2) * PB, PB)

    @pl.when(step == 0)
    def _():
        @pl.when(here)
        def _():
            pltpu.make_async_copy(near_ref.at[pl.ds(half, PB)], right_ref, sem).start()

        @pl.when(jnp.logical_not(here))
        def _():
            pltpu.make_async_copy(far_ref.at[pl.ds(half, PB)], right_ref, sem).start()

        pltpu.make_async_copy(near_ref.at[pl.ds(half, PB)], right_ref, sem).wait()
        high, low = halves(right_ref[...])
        high_ref[...] = high
        low_ref[...] = low

    value = product(halves(left_ref[...]), (high_ref[...], low_ref[...]))
    for yy in range(Y_SIZE):
        for s in range(Y_SIZE):

            @pl.when(lax.rem(yy - y + Y_SIZE, Y_SIZE) == s)
            def _(yy=yy, s=s):
                for zz in range(outs[s].shape[0]):
                    for g in range(4):
                        for l in range(WIDE):
                            row = LANES * zz + 32 * yy + SUBLANES * g
                            outs[s][zz, g * WIDE + l] = value[
                                row : row + SUBLANES, LANES * l : LANES * (l + 1)
                            ]


def at(i, j):
    return slice(LANES * pair(i, j), LANES * (pair(i, j) + 1))


def block(i):
    return slice(LANES * i, LANES * (i + 1))


def solve_kernel(place_ref, *refs):
    mine, other = refs[:Y_SIZE], refs[Y_SIZE : 2 * Y_SIZE]
    x_ref, norm_ref, w = refs[2 * Y_SIZE :]
    r, y = place_ref[0], place_ref[3]
    total = jnp.zeros(TILE, F32)
    for s in range(Y_SIZE):
        source = lax.rem(y - s + Y_SIZE, Y_SIZE)
        for zz in range(mine[s].shape[0]):
            d = zz * Y_SIZE + source
            row = pl.multiple_of(d * SUBLANES, SUBLANES)
            for l in range(WIDE):
                x_ref[pl.ds(row, SUBLANES), block(l)] = mine[s][zz, SLOTS + l]
            for k in range(SLOTS):
                t = d * SLOTS + k
                b, h = t // GROUPS, lax.rem(t, GROUPS)
                spare = b >= len(HALVES[0])
                first = jnp.where(spare, PAIRS, jnp.where(b == 0, 0, b + 5))
                second = jnp.where(spare, PAIRS, b + 1)
                places = (jnp.where(r == 0, first, second), jnp.where(r == 0, second, first))
                for p, ref in zip(places, (mine[s], other[s])):
                    row = pl.multiple_of(p * LANES + h * SUBLANES, SUBLANES)
                    w[pl.ds(row, SUBLANES)] = ref[zz, k]
        here = SUM_PIECE // Y_SIZE, SUM_SLOT
        total = total + jnp.where(source == SUM_PIECE % Y_SIZE, mine[s][here] + other[s][here], 0.0)
    norm_ref[0] = jnp.sqrt(total / 2048.0)[0, 0]

    low = {(i, j): w[at(i, j)] for i in range(BLOCKS) for j in range(i + 1)}
    rows = [x_ref[:, block(l)] for l in range(WIDE)]
    for s in range(BLOCKS):
        parts = [None] * GROUPS

        def load(h, square=low[s, s]):
            return square[SUBLANES * h : SUBLANES * (h + 1)]

        inverse_factor(load, parts.__setitem__)
        inv = jnp.concatenate(parts)
        for i in range(s + 1, BLOCKS):
            low[i, s] = times_transposed(low[i, s], inv)
        for j in range(s + 1, BLOCKS):
            for i in range(j, BLOCKS):
                low[i, j] = low[i, j] - times_transposed(low[i, s], low[j, s])
        x = times_transposed(rows[s], inv)
        x_ref[:, block(s)] = x
        for j in range(s + 1, BLOCKS):
            rows[j] = rows[j] - times_transposed(x, low[j, s])


SMEM = pl.BlockSpec(memory_space=pltpu.SMEM)
VMEM = pl.BlockSpec(memory_space=pltpu.VMEM)
ANY = pl.BlockSpec(memory_space=pl.ANY)


def shaped(*dims):
    return jax.ShapeDtypeStruct(dims, F32)


def call(kernel, flops, outs, in_specs, scratch=(), grid=(), out_spec=None, out_specs=None, room=None):
    out_specs = out_specs or [out_spec or VMEM] * len(outs)
    return pl.pallas_call(
        kernel,
        out_shape=outs,
        grid=grid,
        in_specs=in_specs,
        out_specs=out_specs,
        scratch_shapes=scratch,
        compiler_params=pltpu.CompilerParams(vmem_limit_bytes=room),
        cost_estimate=pl.CostEstimate(flops=flops, bytes_accessed=4_000_000, transcendentals=0),
    )


def exchange(pieces, axis):
    return lax.all_to_all(pieces, axis, split_axis=0, concat_axis=0, tiled=True)


def shifted(value, axis, by):
    size = lax.axis_size(axis)
    return lax.ppermute(value, axis, [(i, (i + by) % size) for i in range(size)])


def delivered(pieces, axis):
    return [pieces[0]] + [shifted(pieces[s], axis, s) for s in range(1, len(pieces))]


def body(a_tile, panels):
    tile_rows, tile_cols = a_tile.shape
    z_size, depth = lax.axis_size(Z), lax.axis_size(DEPTH)
    c_rows = tile_rows // 4
    share = tile_rows // depth
    k_size = panels.shape[1]
    r, c = lax.axis_index("row"), lax.axis_index("col")
    place = jnp.stack([r, c, lax.axis_index(Z), lax.axis_index(Y)]).astype(jnp.int32)
    swap = [(0, 1), (1, 0)]

    far = lax.ppermute(panels, "row", swap)

    piece = shaped(depth, SLOTS + WIDE, *TILE)
    (part,) = call(
        top_kernel,
        8_000_000_000,
        [piece],
        [SMEM, ANY, ANY],
        [
            pltpu.VMEM((c_rows, k_size), F32),
            pltpu.VMEM((PB, k_size), F32),
            pltpu.VMEM((tile_rows, k_size), F32),
            pltpu.VMEM(piece.shape, F32),
            pltpu.SemaphoreType.DMA((5,)),
        ],
        out_specs=[ANY],
    )(place, panels, far)
    got = exchange(part, DEPTH)

    a_sent = call(
        a_kernel,
        1_000_000_000,
        [shaped(2 * SLOTS + WIDE + 1, *TILE)] * 4,
        [SMEM, ANY],
        [
            pltpu.VMEM((2 * SLOTS, *TILE), F32),
            pltpu.VMEM((4, SUBLANES, PB), F32),
            pltpu.VMEM((BLOCKS, LANES, LANES), F32),
            pltpu.SemaphoreType.DMA((2 * SLOTS + 4 + BLOCKS,)),
        ],
    )(place, a_tile)
    a_got = delivered(a_sent, "col")
    a_got = sum(a_got)
    a_other = lax.ppermute(a_got[SLOTS : 2 * SLOTS], "row", [(0, 1)])

    (piece_copies,) = call(
        merge_kernel,
        1_000_000_000,
        [shaped(z_size, SLOTS + WIDE, *TILE)],
        [SMEM, VMEM, VMEM, VMEM],
        room=8 << 20,
    )(place, got, a_got, a_other)
    copies = exchange(piece_copies, Z)
    mine = [copies] + [shifted(copies, Y, s) for s in range(1, Y_SIZE)]
    other = [lax.ppermute(mine[0], "row", swap)]
    other += [lax.ppermute(part, "row", swap) for part in mine[1:]]

    piece = shaped(z_size, 4 * WIDE, *TILE)
    parts = call(
        block_kernel,
        20_000_000_000,
        [piece] * Y_SIZE,
        [SMEM, pl.BlockSpec((PB, k_size), lambda i: (i, 0)), ANY, ANY],
        [
            pltpu.VMEM((PB, k_size), jnp.bfloat16),
            pltpu.VMEM((PB, k_size), jnp.bfloat16),
            pltpu.VMEM((PB, k_size), F32),
            pltpu.SemaphoreType.DMA,
        ],
        grid=(2,),
        out_spec=pl.BlockSpec((z_size // 2, *piece.shape[1:]), lambda i: (i, 0, 0, 0)),
        room=54 << 20,
    )(place, panels, panels, far)
    parts = delivered(parts, Y)
    part = sum(parts)
    got = exchange(part, Z)
    tiles = got.sum(axis=0)
    tiles = tiles.reshape(4, WIDE, *TILE).transpose(0, 2, 1, 3).reshape(share, tile_cols)
    d = lax.axis_index(DEPTH)
    trailing = lax.dynamic_slice_in_dim(a_tile, d * share, share, 0) - tiles

    new_panel, norm = call(
        solve_kernel,
        30_000_000_000,
        [shaped(c_rows, PB), shaped(1)],
        [SMEM] + [VMEM] * (2 * Y_SIZE),
        [pltpu.VMEM(((PAIRS + 1) * LANES, LANES), F32)],
        out_specs=[VMEM, SMEM],
        room=24 << 20,
    )(place, *mine, *other)
    return (trailing, new_panel, norm)


def solution(mesh):
    finer = Mesh(
        mesh.devices.reshape(mesh.shape["row"], mesh.shape["col"], 8, 4),
        ("row", "col", "depth_0", "depth_1"),
    )
    in_specs = (P("row", "col"), P("row", DEPTH))
    out_specs = (P(ROW_DEPTH, "col"), P(("row", "col"), None), P())
    return jax.shard_map(body, mesh=finer, in_specs=in_specs, out_specs=out_specs, check_vma=False)
```
